512 devices in a mesh: row: 64 (over z_hi, y, x), col: 8 (over z_lo, core).
Axes of the slice: x: 4, y: 4, z: 16 (z_hi: 4, z_lo: 4; z = z_hi * 4 + z_lo), core: 2. Of those that a mesh axis runs over, the one named last changes fastest.
Arguments:
- species: float32 [2, 512, 512, 256], P(None, None, 'row', 'col'), may hold values from -6 to 6
- symbol_x: float32 [512], replicated, may hold values from 0.3 to 3
- symbol_y: float32 [512], replicated, may hold values from 0.3 to 3
- symbol_z: float32 [256], replicated, may hold values from 0.3 to 3
Outputs:
- spectrum: float32 [2, 512, 512, 256], P(None, 'row', 'col')
The draws below stay inside these ranges and needn't reach their ends.
All inputs are finite; a program needn't handle non-finite values.
Results may differ from the reference program's by a relative error of at most 0.00007.
Values sent between devices are 32-bit elements; how exact they have to be, the bound alone decides.
A program may use at most 64 MiB of HBM per device.

```python
import jax
import jax.numpy as jnp
from jax import lax

GRID_X = 512
GRID_Y = 512
GRID_Z = 256
FIELDS = 2


def level_of(own_key, extent, split, least, high):
    def one(position, shards_of):
        heights = jax.random.uniform(jax.random.fold_in(jax.random.fold_in(own_key, 6), position), (shards_of,), jnp.float32, least / len(split), high / len(split))
        return jnp.repeat(jnp.exp(heights), extent[position] // shards_of).reshape((-1,) + (1,) * (len(extent) - position - 1))

    level = one(*split[0])
    for cut in split[1:]:
        level = level * one(*cut)
    return level


def centred(rng, shape, scale, most, cuts=(), held_as=jnp.bfloat16):
    entries = jax.random.normal(rng, shape, jnp.float32) * scale
    if len(cuts) > 0:
        entries = level_of(rng, shape, cuts, -0.22, 0.18) * entries
    return jnp.clip(entries, min=-most, max=most).astype(held_as)


def setup_inputs(seed: int = 0) -> dict:
    key_of = jax.random.split(jax.random.key(seed), 5)
    return {
        "species": centred(key_of[0], (FIELDS, GRID_X, GRID_Y, GRID_Z), 1.0, 6.0, ((2, 64), (3, 8)), jnp.float32),
        "symbol_x": jnp.clip(jax.random.uniform(key_of[1], (GRID_X,), jnp.float32, 0.3, 3.0), 0.3, 3.0),
        "symbol_y": jnp.clip(jax.random.uniform(key_of[2], (GRID_Y,), jnp.float32, 0.3, 3.0), 0.3, 3.0),
        "symbol_z": jnp.clip(jax.random.uniform(key_of[3], (GRID_Z,), jnp.float32, 0.3, 3.0), 0.3, 3.0),
    }


def basis_table(count):
    rank = jnp.arange(count)
    angle = (jnp.pi / (4 * count)) * (((2 * rank[:, None] + 1) * (2 * rank[None, :] + 1)) % (8 * count)).astype(jnp.float32)
    return jnp.cos(angle) * (2.0 / count) ** 0.5


def to_modes(values, dim):
    moved = jnp.tensordot(values, basis_table(values.shape[dim]), axes=([dim], [0]), precision=lax.Precision.HIGHEST)
    return jnp.moveaxis(moved, -1, dim)


def reference(species, symbol_x, symbol_y, symbol_z):
    spectrum = species
    spectrum = to_modes(spectrum, 1)
    spectrum = to_modes(spectrum, 2)
    spectrum = to_modes(spectrum, 3)
    symbol = symbol_x[:, None, None] + symbol_y[None, :, None] + symbol_z[None, None, :]
    spectrum = spectrum / symbol
    return spectrum
```

```python
import functools

import jax
import jax.numpy as jnp
import ml_dtypes
import numpy as np
from jax import lax
from jax.experimental import pallas as pl
from jax.experimental.pallas import tpu as pltpu
from jax.sharding import PartitionSpec as P

MESH = pl.DeviceIdType.MESH
F32 = jnp.float32
BF16 = jnp.bfloat16


def split_table(count):
    rank = np.arange(count, dtype=np.float64)
    angle = np.pi / (4 * count) * (2 * rank[:, None] + 1) * (2 * rank[None, :] + 1)
    table = (np.cos(angle) * np.sqrt(2.0 / count)).astype(np.float32)
    high = table.astype(ml_dtypes.bfloat16)
    low = (table - high.astype(np.float32)).astype(ml_dtypes.bfloat16)
    return np.stack([high, low])


def halves(values):
    high = values.astype(BF16)
    return high, (values - high.astype(F32)).astype(BF16)


def product(a, b, dims):
    dot = functools.partial(
        lax.dot_general, dimension_numbers=(dims, ((), ())), preferred_element_type=F32
    )
    return dot(a[0], b[0]) + dot(a[0], b[1]) + dot(a[1], b[0])


def swap_granules(v0, v1):
    sub = lax.broadcasted_iota(jnp.int32, (8, 128), 0)
    lane = lax.broadcasted_iota(jnp.int32, (8, 128), 1)
    upper = sub >= 4
    w0 = jnp.where(upper, pltpu.roll(v1, 4, 0), v0)
    w1 = jnp.where(upper, v1, pltpu.roll(v0, 4, 0))
    s1, g1 = (sub // 2) % 2, lane // 64
    s0, g0 = sub % 2, (lane // 32) % 2
    out = []
    for w in (w0, w1):
        u = pltpu.roll(w, 64, 1)
        w = jnp.where(
            s1 == g1, w, jnp.where(s1 == 0, pltpu.roll(u, 6, 0), pltpu.roll(u, 2, 0))
        )
        a, b = pltpu.roll(w, 32, 1), pltpu.roll(w, 96, 1)
        w = jnp.where(
            s0 == g0, w, jnp.where(s0 == 0, pltpu.roll(a, 7, 0), pltpu.roll(b, 1, 0))
        )
        out.append(w)
    return out


def swap_four(v):
    lane = lax.broadcasted_iota(jnp.int32, (8, 128), 1)
    g1, g0 = lane // 64 == 1, (lane // 32) % 2 == 1
    w = [None] * 4
    for k in range(2):
        a, b = v[k], v[k + 2]
        w[k] = jnp.where(g1, pltpu.roll(b, 64, 1), a)
        w[k + 2] = jnp.where(g1, b, pltpu.roll(a, 64, 1))
    o = [None] * 4
    for k in (0, 2):
        a, b = w[k], w[k + 1]
        o[k] = jnp.where(g0, pltpu.roll(b, 32, 1), a)
        o[k + 1] = jnp.where(g0, b, pltpu.roll(a, 96, 1))
    return o


def kernel(
    rows, cols, x_hbm, h_hbm, hz_hbm, sx_hbm, sy_hbm, sz_hbm, out, symbol,
    x, h, hz, sx, sy, sz, mid, to_row, from_row, to_col, from_col, line,
    load_sem, send_sem, recv_sem,
):
    row, col = lax.axis_index("row"), lax.axis_index("col")
    fields = x.shape[0]

    barrier = pltpu.get_barrier_semaphore()

    @pl.loop(1, rows)
    def _(i):
        peer = (lax.rem(row + i, rows), col)
        pl.semaphore_signal(barrier, inc=1, device_id=peer, device_id_type=MESH)

    @pl.loop(1, cols)
    def _(i):
        peer = (row, lax.rem(col + i, cols))
        pl.semaphore_signal(barrier, inc=1, device_id=peer, device_id_type=MESH)

    loads = [
        pltpu.make_async_copy(src, dst, load_sem.at[k])
        for k, (src, dst) in enumerate(
            [
                (h_hbm, h),
                (x_hbm.at[0], x.at[0]),
                (x_hbm.at[1], x.at[1]),
                (hz_hbm, hz),
                (sx_hbm, sx),
                (sy_hbm, sy),
                (sz_hbm, sz),
            ]
        )
    ]
    for load in loads:
        load.start()
    loads[0].wait()

    def first(f):
        loads[1 + f].wait()
        mid[...] = product((h[0], h[1]), halves(x[f]), ((1,), (1,)))

        @pl.loop(0, rows // 4)
        def _(g):
            for k in range(4):
                peer = g * 4 + k
                at = pl.ds(pl.multiple_of(peer * 8, 8), 8)
                v = swap_granules(mid[at, :128], mid[at, 128:])
                to_row[f, peer, :, :128] = v[0]
                to_row[f, peer, :, 128:] = v[1]

        from_row[f, row] = to_row[f, row]

    def row_copy(f, peer):
        return pltpu.make_async_remote_copy(
            to_row.at[f, peer], from_row.at[f, row], send_sem.at[f], recv_sem.at[f],
            device_id=(peer, col), device_id_type=MESH,
        )

    def send_rows(f):
        @pl.loop(1, rows)
        def _(i):
            row_copy(f, lax.rem(row + i, rows)).start()

    def all_rows(f):
        return pltpu.make_async_remote_copy(
            to_row.at[f, pl.ds(0, rows - 1)], from_row.at[f, pl.ds(0, rows - 1)],
            send_sem.at[f], recv_sem.at[f],
            device_id=(lax.rem(row + 1, rows), col), device_id_type=MESH,
        )

    def second(f):
        lines = from_row[f].reshape(rows * 8, 256)
        modes = product((h[0], h[1]), halves(lines), ((1,), (0,)))
        to_col[f] = modes.reshape(cols, 64, 256)
        from_col[f, col] = to_col[f, col]

    def send_cols(f):
        for i in range(1, cols):
            peer = lax.rem(col + i, cols)
            pltpu.make_async_remote_copy(
                to_col.at[f, peer], from_col.at[f, col],
                send_sem.at[2 + f], recv_sem.at[2 + f],
                device_id=(row, peer), device_id_type=MESH,
            ).start()

    def all_cols(f):
        return pltpu.make_async_remote_copy(
            to_col.at[f, pl.ds(0, cols - 1)], from_col.at[f, pl.ds(0, cols - 1)],
            send_sem.at[2 + f], recv_sem.at[2 + f],
            device_id=(row, lax.rem(col + 1, cols)), device_id_type=MESH,
        )

    def third(f):
        @pl.loop(0, 8)
        def _(g):
            at = pl.ds(pl.multiple_of(g * 8, 8), 8)
            for i in range(2):
                for j in range(2):
                    lanes, to = pl.ds(128 * i, 128), pl.ds(128 * j, 128)
                    v = swap_four([from_col[f, 4 * j + c, at, lanes] for c in range(4)])
                    for k in range(4):
                        line[4 * i + k, at, to] = v[k]

        lines = line[...].reshape(512, 256)
        modes = product(halves(lines), (hz[0], hz[1]), ((1,), (0,)))
        out[f] = modes.reshape(8, 64, 256)

    def fill_symbol():
        share_x, share_y = symbol.shape[0], symbol.shape[1]
        lane = lax.broadcasted_iota(jnp.int32, (share_y, sy.shape[1]), 1)
        sub = lax.broadcasted_iota(jnp.int32, (share_y, sy.shape[1]), 0)
        mine = lane == col * share_y + sub
        part_y = jnp.sum(jnp.where(mine, sy[...], 0.0), axis=1, keepdims=True)
        lane_x = lax.broadcasted_iota(jnp.int32, sx.shape, 1)
        for k in range(share_x):
            mine = lane_x == row * share_x + k
            part_x = jnp.sum(jnp.where(mine, sx[...], 0.0), axis=1, keepdims=True)
            symbol[k] = (part_x + part_y) + sz[...]

    first(0)
    pl.semaphore_wait(barrier, rows + cols - 2)
    for f in range(fields):
        if f > 0:
            first(f)
        send_rows(f)
    for load in loads[3:]:
        load.wait()
    fill_symbol()
    for f in range(fields):
        all_rows(f).wait_recv()
        second(f)
        send_cols(f)
    for f in range(fields):
        all_cols(f).wait_recv()
        third(f)
    for f in range(fields):
        all_rows(f).wait_send()
        all_cols(f).wait_send()


def on_device(rows, cols, species, symbol_x, symbol_y, symbol_z):
    fields, nx, ny, nz = species.shape
    values = species.transpose(0, 2, 3, 1).reshape(fields, ny * nz, nx)
    table, table_z = jnp.asarray(split_table(nx)), jnp.asarray(split_table(nz * cols))
    share_x, share_y = nx // rows, ny * rows // cols
    anywhere = pl.BlockSpec(memory_space=pl.ANY)
    spectrum, symbol = pl.pallas_call(
        functools.partial(kernel, rows, cols),
        out_shape=[
            jax.ShapeDtypeStruct((fields, share_x, share_y, nz * cols), F32),
            jax.ShapeDtypeStruct((share_x, share_y, nz * cols), F32),
        ],
        in_specs=[anywhere] * 6,
        out_specs=[pl.BlockSpec(memory_space=pltpu.VMEM)] * 2,
        scratch_shapes=[
            pltpu.VMEM(values.shape, F32),
            pltpu.VMEM(table.shape, BF16),
            pltpu.VMEM(table_z.shape, BF16),
            pltpu.VMEM((1, nx), F32),
            pltpu.VMEM((1, ny * rows), F32),
            pltpu.VMEM((1, nz * cols), F32),
            pltpu.VMEM((nx, ny * nz), F32),
            pltpu.VMEM((fields, rows, 8, 256), F32),
            pltpu.VMEM((fields, rows, 8, 256), F32),
            pltpu.VMEM((fields, cols, 64, 256), F32),
            pltpu.VMEM((fields, cols, 64, 256), F32),
            pltpu.VMEM((8, 64, 256), F32),
            pltpu.SemaphoreType.DMA((7,)),
            pltpu.SemaphoreType.DMA((4,)),
            pltpu.SemaphoreType.DMA((4,)),
        ],
        compiler_params=pltpu.CompilerParams(
            collective_id=0, has_side_effects=True, vmem_limit_bytes=60 * 2**20
        ),
    )(values, table, table_z, symbol_x[None], symbol_y[None], symbol_z[None])
    return spectrum / symbol


def solution(mesh):
    in_specs = (P(None, None, "row", "col"), P(), P(), P())
    out_specs = P(None, "row", "col", None)
    return jax.shard_map(
        functools.partial(on_device, mesh.shape["row"], mesh.shape["col"]),
        mesh=mesh, in_specs=in_specs, out_specs=out_specs, check_vma=False,
    )
```

```python
import functools

import jax
import jax.numpy as jnp
import ml_dtypes
import numpy as np
from jax import lax
from jax.experimental import pallas as pl
from jax.experimental.pallas import tpu as pltpu
from jax.sharding import PartitionSpec as P

MESH = pl.DeviceIdType.MESH
F32 = jnp.float32
BF16 = jnp.bfloat16
GROUPS = 4


def split_table(count):
    rank = np.arange(count, dtype=np.float64)
    angle = np.pi / (4 * count) * (2 * rank[:, None] + 1) * (2 * rank[None, :] + 1)
    table = (np.cos(angle) * np.sqrt(2.0 / count)).astype(np.float32)
    high = table.astype(ml_dtypes.bfloat16)
    low = (table - high.astype(np.float32)).astype(ml_dtypes.bfloat16)
    return np.stack([high, low])


def halves(values):
    high = values.astype(BF16)
    return high, (values - high.astype(F32)).astype(BF16)


def product(a, b, dims):
    dot = functools.partial(
        lax.dot_general, dimension_numbers=(dims, ((), ())), preferred_element_type=F32
    )
    return dot(a[0], b[0]) + dot(a[0], b[1]) + dot(a[1], b[0])


def swap_granules(v0, v1):
    sub = lax.broadcasted_iota(jnp.int32, (8, 128), 0)
    lane = lax.broadcasted_iota(jnp.int32, (8, 128), 1)
    upper = sub >= 4
    w0 = jnp.where(upper, pltpu.roll(v1, 4, 0), v0)
    w1 = jnp.where(upper, v1, pltpu.roll(v0, 4, 0))
    s1, g1 = (sub // 2) % 2, lane // 64
    s0, g0 = sub % 2, (lane // 32) % 2
    out = []
    for w in (w0, w1):
        u = pltpu.roll(w, 64, 1)
        w = jnp.where(
            s1 == g1, w, jnp.where(s1 == 0, pltpu.roll(u, 6, 0), pltpu.roll(u, 2, 0))
        )
        a, b = pltpu.roll(w, 32, 1), pltpu.roll(w, 96, 1)
        w = jnp.where(
            s0 == g0, w, jnp.where(s0 == 0, pltpu.roll(a, 7, 0), pltpu.roll(b, 1, 0))
        )
        out.append(w)
    return out


def swap_four(v):
    lane = lax.broadcasted_iota(jnp.int32, (8, 128), 1)
    g1, g0 = lane // 64 == 1, (lane // 32) % 2 == 1
    w = [None] * 4
    for k in range(2):
        a, b = v[k], v[k + 2]
        w[k] = jnp.where(g1, pltpu.roll(b, 64, 1), a)
        w[k + 2] = jnp.where(g1, b, pltpu.roll(a, 64, 1))
    o = [None] * 4
    for k in (0, 2):
        a, b = w[k], w[k + 1]
        o[k] = jnp.where(g0, pltpu.roll(b, 32, 1), a)
        o[k + 1] = jnp.where(g0, b, pltpu.roll(a, 96, 1))
    return o


def kernel(
    rows, cols, x_hbm, h_hbm, hz_hbm, sx_hbm, sy_hbm, sz_hbm, out, symbol,
    x, h, hz, sx, sy, sz, mid, to_row, via, from_row, to_col, from_col, line,
    load_sem, send_sem, recv_sem, z_send_sem, z_recv_sem, ready_sem,
):
    row, col = lax.axis_index("row"), lax.axis_index("col")
    plane = rows // GROUPS
    group, place = row // plane, lax.rem(row, plane)

    def in_group(step):
        return lax.rem(group + step, GROUPS) * plane

    def signal(semaphore, peer):
        pl.semaphore_signal(semaphore, inc=1, device_id=peer, device_id_type=MESH)

    barrier = pltpu.get_barrier_semaphore()
    for step in (1, GROUPS - 1):
        signal(barrier, (in_group(step) + place, col))

    @pl.loop(1, plane)
    def _(i):
        signal(barrier, (in_group(0) + lax.rem(place + i, plane), col))

    @pl.loop(1, cols)
    def _(i):
        signal(barrier, (row, lax.rem(col + i, cols)))

    loads = [
        pltpu.make_async_copy(src, dst, load_sem.at[k])
        for k, (src, dst) in enumerate(
            [
                (h_hbm, h),
                (x_hbm.at[0], x.at[0]),
                (x_hbm.at[1], x.at[1]),
                (hz_hbm, hz),
                (sx_hbm, sx),
                (sy_hbm, sy),
                (sz_hbm, sz),
            ]
        )
    ]
    for load in loads:
        load.start()
    loads[0].wait()

    def first(f):
        loads[1 + f].wait()
        mid[...] = product((h[0], h[1]), halves(x[f]), ((1,), (1,)))

        @pl.loop(0, rows // 4)
        def _(g):
            for k in range(4):
                peer = g * 4 + k
                at = pl.ds(pl.multiple_of(peer * 8, 8), 8)
                v = swap_granules(mid[at, :128], mid[at, 128:])
                to_row[f, peer, :, :128] = v[0]
                to_row[f, peer, :, 128:] = v[1]

    def z_copy(f, step):
        k = f * 3 + step - 1
        return pltpu.make_async_remote_copy(
            to_row.at[f, pl.ds(in_group(step), plane)], via.at[f, step - 1],
            z_send_sem.at[k], z_recv_sem.at[k],
            device_id=(in_group(step) + place, col), device_id_type=MESH,
        )

    def send_plane(f, step):
        source = in_group(GROUPS - step) + place if step else row

        def block(q):
            return via.at[f, step - 1, q] if step else to_row.at[f, row - place + q]

        @pl.loop(1, plane)
        def _(i):
            q = lax.rem(place + i, plane)
            pltpu.make_async_remote_copy(
                block(q), from_row.at[f, source], send_sem.at[f], recv_sem.at[f],
                device_id=(in_group(0) + q, col), device_id_type=MESH,
            ).start()

        from_row[f, source] = block(place)[...]

    def all_rows(f):
        count = GROUPS * (plane - 1)
        return pltpu.make_async_remote_copy(
            to_row.at[f, pl.ds(0, count)], from_row.at[f, pl.ds(0, count)],
            send_sem.at[f], recv_sem.at[f],
            device_id=(in_group(1) + place, col), device_id_type=MESH,
        )

    def second(f):
        lines = from_row[f].reshape(rows * 8, 256)
        modes = product((h[0], h[1]), halves(lines), ((1,), (0,)))
        to_col[f] = modes.reshape(cols, 64, 256)
        from_col[f, col] = to_col[f, col]

    def send_cols(f):
        for i in range(1, cols):
            peer = lax.rem(col + i, cols)
            pltpu.make_async_remote_copy(
                to_col.at[f, peer], from_col.at[f, col],
                send_sem.at[2 + f], recv_sem.at[2 + f],
                device_id=(row, peer), device_id_type=MESH,
            ).start()

    def all_cols(f):
        return pltpu.make_async_remote_copy(
            to_col.at[f, pl.ds(0, cols - 1)], from_col.at[f, pl.ds(0, cols - 1)],
            send_sem.at[2 + f], recv_sem.at[2 + f],
            device_id=(row, lax.rem(col + 1, cols)), device_id_type=MESH,
        )

    def third(f):
        @pl.loop(0, 8)
        def _(g):
            at = pl.ds(pl.multiple_of(g * 8, 8), 8)
            for i in range(2):
                for j in range(2):
                    lanes, to = pl.ds(128 * i, 128), pl.ds(128 * j, 128)
                    v = swap_four([from_col[f, 4 * j + c, at, lanes] for c in range(4)])
                    for k in range(4):
                        line[4 * i + k, at, to] = v[k]

        lines = line[...].reshape(512, 256)
        modes = product(halves(lines), (hz[0], hz[1]), ((1,), (0,)))
        out[f] = modes.reshape(8, 64, 256)

    def fill_symbol():
        share_x, share_y = symbol.shape[0], symbol.shape[1]
        lane = lax.broadcasted_iota(jnp.int32, (share_y, sy.shape[1]), 1)
        sub = lax.broadcasted_iota(jnp.int32, (share_y, sy.shape[1]), 0)
        mine = lane == col * share_y + sub
        part_y = jnp.sum(jnp.where(mine, sy[...], 0.0), axis=1, keepdims=True)
        lane_x = lax.broadcasted_iota(jnp.int32, sx.shape, 1)
        for k in range(share_x):
            mine = lane_x == row * share_x + k
            part_x = jnp.sum(jnp.where(mine, sx[...], 0.0), axis=1, keepdims=True)
            symbol[k] = (part_x + part_y) + sz[...]

    near = (1, GROUPS - 1)
    first(0)
    pl.semaphore_wait(barrier, plane + cols)
    for step in near:
        z_copy(0, step).start()
    for step in near:
        signal(ready_sem, (in_group(step) + place, col))
    send_plane(0, 0)
    first(1)
    pl.semaphore_wait(ready_sem, 2)
    z_copy(0, 2).start()
    for step in (*near, 2):
        z_copy(1, step).start()
    send_plane(1, 0)
    for load in loads[3:]:
        load.wait()
    fill_symbol()
    for f in range(2):
        for step in (*near, 2):
            z_copy(f, step).wait_recv()
            send_plane(f, step)
        all_rows(f).wait_recv()
        second(f)
        send_cols(f)
    for f in range(2):
        all_cols(f).wait_recv()
        third(f)
    for f in range(2):
        for step in (*near, 2):
            z_copy(f, step).wait_send()
        all_rows(f).wait_send()
        all_cols(f).wait_send()


def on_device(rows, cols, species, symbol_x, symbol_y, symbol_z):
    fields, nx, ny, nz = species.shape
    values = species.transpose(0, 2, 3, 1).reshape(fields, ny * nz, nx)
    table, table_z = jnp.asarray(split_table(nx)), jnp.asarray(split_table(nz * cols))
    share_x, share_y = nx // rows, ny * rows // cols
    anywhere = pl.BlockSpec(memory_space=pl.ANY)
    spectrum, symbol = pl.pallas_call(
        functools.partial(kernel, rows, cols),
        out_shape=[
            jax.ShapeDtypeStruct((fields, share_x, share_y, nz * cols), F32),
            jax.ShapeDtypeStruct((share_x, share_y, nz * cols), F32),
        ],
        in_specs=[anywhere] * 6,
        out_specs=[pl.BlockSpec(memory_space=pltpu.VMEM)] * 2,
        scratch_shapes=[
            pltpu.VMEM(values.shape, F32),
            pltpu.VMEM(table.shape, BF16),
            pltpu.VMEM(table_z.shape, BF16),
            pltpu.VMEM((1, nx), F32),
            pltpu.VMEM((1, ny * rows), F32),
            pltpu.VMEM((1, nz * cols), F32),
            pltpu.VMEM((nx, ny * nz), F32),
            pltpu.VMEM((fields, rows, 8, 256), F32),
            pltpu.VMEM((fields, GROUPS - 1, rows // GROUPS, 8, 256), F32),
            pltpu.VMEM((fields, rows, 8, 256), F32),
            pltpu.VMEM((fields, cols, 64, 256), F32),
            pltpu.VMEM((fields, cols, 64, 256), F32),
            pltpu.VMEM((8, 64, 256), F32),
            pltpu.SemaphoreType.DMA((7,)),
            pltpu.SemaphoreType.DMA((4,)),
            pltpu.SemaphoreType.DMA((4,)),
            pltpu.SemaphoreType.DMA((6,)),
            pltpu.SemaphoreType.DMA((6,)),
            pltpu.SemaphoreType.REGULAR,
        ],
        compiler_params=pltpu.CompilerParams(
            collective_id=0, has_side_effects=True, vmem_limit_bytes=60 * 2**20
        ),
    )(values, table, table_z, symbol_x[None], symbol_y[None], symbol_z[None])
    return spectrum / symbol


def solution(mesh):
    in_specs = (P(None, None, "row", "col"), P(), P(), P())
    out_specs = P(None, "row", "col", None)
    return jax.shard_map(
        functools.partial(on_device, mesh.shape["row"], mesh.shape["col"]),
        mesh=mesh, in_specs=in_specs, out_specs=out_specs, check_vma=False,
    )
```

```python
import functools

import jax
import jax.numpy as jnp
import ml_dtypes
import numpy as np
from jax import lax
from jax.experimental import pallas as pl
from jax.experimental.pallas import tpu as pltpu
from jax.sharding import PartitionSpec as P

MESH = pl.DeviceIdType.MESH
F32 = jnp.float32
BF16 = jnp.bfloat16
GROUPS = 4
VMEM_LIMIT = 53500 * 2**10


def split_table(count):
    rank = np.arange(count, dtype=np.float64)
    angle = np.pi / (4 * count) * (2 * rank[:, None] + 1) * (2 * rank[None, :] + 1)
    table = (np.cos(angle) * np.sqrt(2.0 / count)).astype(np.float32)
    high = table.astype(ml_dtypes.bfloat16)
    low = (table - high.astype(np.float32)).astype(ml_dtypes.bfloat16)
    return np.stack([high, low])


def halves(values):
    high = values.astype(BF16)
    return high, (values - high.astype(F32)).astype(BF16)


def product(a, b, dims):
    dot = functools.partial(
        lax.dot_general, dimension_numbers=(dims, ((), ())), preferred_element_type=F32
    )
    return dot(a[0], b[0]) + dot(a[0], b[1]) + dot(a[1], b[0])


def swap_granules(v0, v1):
    sub = lax.broadcasted_iota(jnp.int32, (8, 128), 0)
    lane = lax.broadcasted_iota(jnp.int32, (8, 128), 1)
    upper = sub >= 4
    w0 = jnp.where(upper, pltpu.roll(v1, 4, 0), v0)
    w1 = jnp.where(upper, v1, pltpu.roll(v0, 4, 0))
    s1, g1 = (sub // 2) % 2, lane // 64
    s0, g0 = sub % 2, (lane // 32) % 2
    out = []
    for w in (w0, w1):
        u = pltpu.roll(w, 64, 1)
        w = jnp.where(
            s1 == g1, w, jnp.where(s1 == 0, pltpu.roll(u, 6, 0), pltpu.roll(u, 2, 0))
        )
        a, b = pltpu.roll(w, 32, 1), pltpu.roll(w, 96, 1)
        w = jnp.where(
            s0 == g0, w, jnp.where(s0 == 0, pltpu.roll(a, 7, 0), pltpu.roll(b, 1, 0))
        )
        out.append(w)
    return out


def swap_four(v):
    lane = lax.broadcasted_iota(jnp.int32, (8, 128), 1)
    g1, g0 = lane // 64 == 1, (lane // 32) % 2 == 1
    w = [None] * 4
    for k in range(2):
        a, b = v[k], v[k + 2]
        w[k] = jnp.where(g1, pltpu.roll(b, 64, 1), a)
        w[k + 2] = jnp.where(g1, b, pltpu.roll(a, 64, 1))
    o = [None] * 4
    for k in (0, 2):
        a, b = w[k], w[k + 1]
        o[k] = jnp.where(g0, pltpu.roll(b, 32, 1), a)
        o[k + 1] = jnp.where(g0, b, pltpu.roll(a, 96, 1))
    return o


def kernel(
    rows, cols, x_hbm, h_hbm, out, x, xs, h, hz, mid, to_row, via, from_row, to_col, from_col, line,
    load_sem, send_sem, recv_sem, z_send_sem, z_recv_sem, ready_sem,
):
    row, col = lax.axis_index("row"), lax.axis_index("col")
    plane = rows // GROUPS
    group, place = row // plane, lax.rem(row, plane)

    def in_group(step):
        return lax.rem(group + step, GROUPS) * plane

    def signal(semaphore, peer):
        pl.semaphore_signal(semaphore, inc=1, device_id=peer, device_id_type=MESH)

    barrier = pltpu.get_barrier_semaphore()
    for step in (1, GROUPS - 1):
        signal(barrier, (in_group(step) + place, col))

    @pl.loop(1, plane)
    def _(i):
        signal(barrier, (in_group(0) + lax.rem(place + i, plane), col))

    @pl.loop(1, cols)
    def _(i):
        signal(barrier, (row, lax.rem(col + i, cols)))

    def table_part(step):
        at = pl.ds(pl.multiple_of(in_group(step) * 8, 128), plane * 8)
        return h_hbm.at[:, at, :], h.at[:, at, :]

    near = (1, GROUPS - 1)
    sources = [
        (x_hbm.at[0], x.at[0]),
        table_part(1),
        table_part(GROUPS - 1),
        table_part(2),
        table_part(0),
        (x_hbm.at[1], x.at[1]),
        (h_hbm.at[:, pl.ds(x.shape[2], hz.shape[1]), pl.ds(0, hz.shape[1])], hz),
    ]
    loads = [
        pltpu.make_async_copy(src, dst, load_sem.at[k])
        for k, (src, dst) in enumerate(sources)
    ]
    for load in loads:
        load.start()

    def first(f, step):
        top = pl.multiple_of(in_group(step) * 8, 128)
        at = pl.ds(top, plane * 8)
        mid[...] = product((h[0, at], h[1, at]), (xs[f, 0], xs[f, 1]), ((1,), (1,)))

        @pl.loop(0, plane // 4)
        def _(g):
            for k in range(4):
                here = pl.ds(pl.multiple_of((g * 4 + k) * 8, 8), 8)
                v = swap_granules(mid[here, :128], mid[here, 128:])
                to_row[f, in_group(step) + g * 4 + k, :, :128] = v[0]
                to_row[f, in_group(step) + g * 4 + k, :, 128:] = v[1]

    def split(f):
        xs[f, 0], xs[f, 1] = halves(x[f])

    def z_copy(f, step):
        k = f * 3 + step - 1
        return pltpu.make_async_remote_copy(
            to_row.at[f, pl.ds(in_group(step), plane)], via.at[f, step - 1],
            z_send_sem.at[k], z_recv_sem.at[k],
            device_id=(in_group(step) + place, col), device_id_type=MESH,
        )

    def send_plane(f, step):
        source = in_group(GROUPS - step) + place if step else row

        def block(q):
            return via.at[f, step - 1, q] if step else to_row.at[f, row - place + q]

        @pl.loop(1, plane)
        def _(i):
            q = lax.rem(place + i, plane)
            pltpu.make_async_remote_copy(
                block(q), from_row.at[f, source], send_sem.at[f], recv_sem.at[f],
                device_id=(in_group(0) + q, col), device_id_type=MESH,
            ).start()

        from_row[f, source] = block(place)[...]

    def all_rows(f):
        count = GROUPS * (plane - 1)
        return pltpu.make_async_remote_copy(
            to_row.at[f, pl.ds(0, count)], from_row.at[f, pl.ds(0, count)],
            send_sem.at[f], recv_sem.at[f],
            device_id=(in_group(1) + place, col), device_id_type=MESH,
        )

    def second(f):
        lines = from_row[f].reshape(rows * 8, 256)
        modes = product((h[0], h[1]), halves(lines), ((1,), (0,)))
        for part in range(2):
            lanes = slice(128 * part, 128 * part + 128)
            to_col[f, part] = modes[:, lanes].reshape(cols, 64, 128)
            from_col[f, part, col] = to_col[f, part, col]

    def send_cols(f, part):
        for i in range(1, cols):
            peer = lax.rem(col + i, cols)
            pltpu.make_async_remote_copy(
                to_col.at[f, part, peer], from_col.at[f, part, col],
                send_sem.at[2 + 2 * f + part], recv_sem.at[2 + 2 * f + part],
                device_id=(row, peer), device_id_type=MESH,
            ).start()

    def all_cols(f, part):
        return pltpu.make_async_remote_copy(
            to_col.at[f, part, pl.ds(0, cols - 1)],
            from_col.at[f, part, pl.ds(0, cols - 1)],
            send_sem.at[2 + 2 * f + part], recv_sem.at[2 + 2 * f + part],
            device_id=(row, lax.rem(col + 1, cols)), device_id_type=MESH,
        )

    def third(f, part):
        @pl.loop(0, 8)
        def _(g):
            at = pl.ds(pl.multiple_of(g * 8, 8), 8)
            for j in range(2):
                v = swap_four([from_col[f, part, 4 * j + c, at] for c in range(4)])
                for k in range(4):
                    line[k, at, pl.ds(128 * j, 128)] = v[k]

        lines = line[...].reshape(256, 256)
        modes = product(halves(lines), (hz[0], hz[1]), ((1,), (0,)))
        out[f, 4 * part : 4 * part + 4] = modes.reshape(4, 64, 256)

    loads[0].wait()
    split(0)
    for k, step in enumerate((*near, 2, 0)):
        loads[1 + k].wait()
        first(0, step)
        if k == 0:
            pl.semaphore_wait(barrier, plane + cols)
            for other in near:
                signal(ready_sem, (in_group(other) + place, col))
        if step in near:
            z_copy(0, step).start()
    send_plane(0, 0)
    pl.semaphore_wait(ready_sem, 2)
    z_copy(0, 2).start()
    loads[5].wait()
    split(1)
    for step in (*near, 2, 0):
        first(1, step)
        if step:
            z_copy(1, step).start()
    send_plane(1, 0)
    loads[6].wait()
    for f in range(2):
        for step in (*near, 2):
            z_copy(f, step).wait_recv()
            send_plane(f, step)
        all_rows(f).wait_recv()
        second(f)
        for part in range(2):
            send_cols(f, part)
    for f in range(2):
        for part in range(2):
            all_cols(f, part).wait_recv()
            third(f, part)
    for f in range(2):
        for step in (*near, 2):
            z_copy(f, step).wait_send()
        all_rows(f).wait_send()
        for part in range(2):
            all_cols(f, part).wait_send()


def divide(spectrum, sx, sy, sz, out, done, sems):
    row, col = lax.axis_index("row"), lax.axis_index("col")
    fields, share_x, share_y, nz = spectrum.shape
    lane = lax.broadcasted_iota(jnp.int32, (share_y, sy.shape[1]), 1)
    sub = lax.broadcasted_iota(jnp.int32, (share_y, sy.shape[1]), 0)
    mine = lane == col * share_y + sub
    part_y = jnp.sum(jnp.where(mine, sy[...], 0.0), axis=1, keepdims=True)
    lane_x = lax.broadcasted_iota(jnp.int32, sx.shape, 1)
    copies = []
    for k in range(share_x):
        mine = lane_x == row * share_x + k
        part_x = jnp.sum(jnp.where(mine, sx[...], 0.0), axis=1, keepdims=True)
        symbol = (part_x + part_y) + sz[...]
        for f in range(fields):
            done[f, k] = spectrum[f, k] / symbol
        if k % 2 == 1:
            two = pl.ds(k - 1, 2)
            copies.append(
                pltpu.make_async_copy(done.at[:, two], out.at[:, two], sems.at[k // 2])
            )
            copies[-1].start()
    for copy in copies:
        copy.wait()


def on_device(rows, cols, species, symbol_x, symbol_y, symbol_z):
    fields, nx, ny, nz = species.shape
    values = species.transpose(0, 2, 3, 1).reshape(fields, ny * nz, nx)
    table_z = np.pad(split_table(nz * cols), ((0, 0), (0, 0), (0, nx - nz * cols)))
    table = jnp.asarray(np.concatenate([split_table(nx), table_z], axis=1))
    share_x, share_y = nx // rows, ny * rows // cols
    in_hbm = pl.BlockSpec(memory_space=pltpu.HBM)
    in_vmem = pl.BlockSpec(memory_space=pltpu.VMEM)
    result = jax.ShapeDtypeStruct((fields, share_x, share_y, nz * cols), F32)
    spectrum = pl.pallas_call(
        functools.partial(kernel, rows, cols),
        out_shape=result,
        in_specs=[in_hbm] * 2,
        out_specs=in_vmem,
        scratch_shapes=[
            pltpu.VMEM(values.shape, F32),
            pltpu.VMEM((fields, 2, ny * nz, nx), BF16),
            pltpu.VMEM((2, nx, nx), BF16),
            pltpu.VMEM((2, nz * cols, nz * cols), BF16),
            pltpu.VMEM((nx // GROUPS, ny * nz), F32),
            pltpu.VMEM((fields, rows, 8, 256), F32),
            pltpu.VMEM((fields, GROUPS - 1, rows // GROUPS, 8, 256), F32),
            pltpu.VMEM((fields, rows, 8, 256), F32),
            pltpu.VMEM((fields, 2, cols, 64, 128), F32),
            pltpu.VMEM((fields, 2, cols, 64, 128), F32),
            pltpu.VMEM((4, 64, 256), F32),
            pltpu.SemaphoreType.DMA((7,)),
            pltpu.SemaphoreType.DMA((6,)),
            pltpu.SemaphoreType.DMA((6,)),
            pltpu.SemaphoreType.DMA((6,)),
            pltpu.SemaphoreType.DMA((6,)),
            pltpu.SemaphoreType.REGULAR,
        ],
        compiler_params=pltpu.CompilerParams(
            collective_id=0, has_side_effects=True, vmem_limit_bytes=VMEM_LIMIT
        ),
    )(values, table)
    return pl.pallas_call(
        divide,
        out_shape=result,
        in_specs=[in_vmem] * 4,
        out_specs=in_hbm,
        scratch_shapes=[
            pltpu.VMEM(result.shape, F32),
            pltpu.SemaphoreType.DMA((share_x // 2,)),
        ],
        compiler_params=pltpu.CompilerParams(vmem_limit_bytes=8 * 2**20),
    )(spectrum, symbol_x[None], symbol_y[None], symbol_z[None])


def solution(mesh):
    in_specs = (P(None, None, "row", "col"), P(), P(), P())
    out_specs = P(None, "row", "col", None)
    return jax.shard_map(
        functools.partial(on_device, mesh.shape["row"], mesh.shape["col"]),
        mesh=mesh, in_specs=in_specs, out_specs=out_specs, check_vma=False,
    )
```

```python
import functools

import jax
import jax.numpy as jnp
import ml_dtypes
import numpy as np
from jax import lax
from jax.experimental import pallas as pl
from jax.experimental.pallas import tpu as pltpu
from jax.sharding import PartitionSpec as P

MESH = pl.DeviceIdType.MESH
F32 = jnp.float32
BF16 = jnp.bfloat16
GROUPS = 4
VMEM_LIMIT = 53500 * 2**10


def split_table(count):
    rank = np.arange(count, dtype=np.float64)
    angle = np.pi / (4 * count) * (2 * rank[:, None] + 1) * (2 * rank[None, :] + 1)
    table = (np.cos(angle) * np.sqrt(2.0 / count)).astype(np.float32)
    high = table.astype(ml_dtypes.bfloat16)
    low = (table - high.astype(np.float32)).astype(ml_dtypes.bfloat16)
    return np.stack([high, low])


def halves(values):
    high = values.astype(BF16)
    return high, (values - high.astype(F32)).astype(BF16)


def product(a, b, dims):
    dot = functools.partial(
        lax.dot_general, dimension_numbers=(dims, ((), ())), preferred_element_type=F32
    )
    return dot(a[0], b[0]) + dot(a[0], b[1]) + dot(a[1], b[0])


def swap_granules(v0, v1):
    sub = lax.broadcasted_iota(jnp.int32, (8, 128), 0)
    lane = lax.broadcasted_iota(jnp.int32, (8, 128), 1)
    upper = sub >= 4
    w0 = jnp.where(upper, pltpu.roll(v1, 4, 0), v0)
    w1 = jnp.where(upper, v1, pltpu.roll(v0, 4, 0))
    s1, g1 = (sub // 2) % 2, lane // 64
    s0, g0 = sub % 2, (lane // 32) % 2
    out = []
    for w in (w0, w1):
        u = pltpu.roll(w, 64, 1)
        w = jnp.where(
            s1 == g1, w, jnp.where(s1 == 0, pltpu.roll(u, 6, 0), pltpu.roll(u, 2, 0))
        )
        a, b = pltpu.roll(w, 32, 1), pltpu.roll(w, 96, 1)
        w = jnp.where(
            s0 == g0, w, jnp.where(s0 == 0, pltpu.roll(a, 7, 0), pltpu.roll(b, 1, 0))
        )
        out.append(w)
    return out


def swap_four(v):
    lane = lax.broadcasted_iota(jnp.int32, (8, 128), 1)
    g1, g0 = lane // 64 == 1, (lane // 32) % 2 == 1
    w = [None] * 4
    for k in range(2):
        a, b = v[k], v[k + 2]
        w[k] = jnp.where(g1, pltpu.roll(b, 64, 1), a)
        w[k + 2] = jnp.where(g1, b, pltpu.roll(a, 64, 1))
    o = [None] * 4
    for k in (0, 2):
        a, b = w[k], w[k + 1]
        o[k] = jnp.where(g0, pltpu.roll(b, 32, 1), a)
        o[k + 1] = jnp.where(g0, b, pltpu.roll(a, 96, 1))
    return o


def kernel(
    rows, cols, x_hbm, h_hbm, out, x, xs, h, hz, mid, to_row, via, from_row, to_col, from_col, line,
    load_sem, send_sem, recv_sem, z_send_sem, z_recv_sem, ready_sem, round_sem,
):
    row, col = lax.axis_index("row"), lax.axis_index("col")
    plane = rows // GROUPS
    group, place = row // plane, lax.rem(row, plane)

    def in_group(step):
        return lax.rem(group + step, GROUPS) * plane

    def signal(semaphore, peer):
        pl.semaphore_signal(semaphore, inc=1, device_id=peer, device_id_type=MESH)

    def in_plane(x_step, y_step):
        x = lax.rem(lax.rem(place, 4) + x_step, 4)
        y = lax.rem(place // 4 + y_step, 4)
        return row - place + 4 * y + x, col

    flip = lax.rem(group % 2 + group // 2, 2)
    step_a, step_b = 1 + 2 * flip, 3 - 2 * flip
    peer_a = (in_group(step_a) + place, col)
    peer_b = (in_group(step_b) + place, col)
    z_lo = col // 2
    adjacent = [
        in_plane(1, 0),
        in_plane(3, 0),
        in_plane(0, 1),
        in_plane(0, 3),
        (row, col + 1 - 2 * lax.rem(col, 2)),
    ]
    n_adjacent = len(adjacent) + 1 + z_lo * (3 - z_lo) // 2

    def signal_adjacent(semaphore):
        for peer in adjacent:
            signal(semaphore, peer)

        @pl.when(z_lo > 0)
        def _():
            signal(semaphore, (row, col - 2))

        @pl.when(z_lo < 3)
        def _():
            signal(semaphore, (row, col + 2))

    barrier = pltpu.get_barrier_semaphore()
    n_lower = group % 2 + 2 * (group // 2) * (1 - group % 2)

    @pl.when(group == 0)
    def _():
        signal(barrier, peer_a)

    @pl.when(group != 2)
    def _():
        signal(barrier, peer_b)

    signal_adjacent(barrier)

    def answer():
        @pl.when(group == 1)
        def _():
            signal(ready_sem.at[0], peer_a)

        @pl.when(group >= 2)
        def _():
            signal(ready_sem.at[1], peer_a)

        @pl.when(group == 2)
        def _():
            signal(ready_sem.at[1], peer_b)

    def tell(k):
        signal_adjacent(round_sem.at[k])

    def hear(k):
        pl.semaphore_wait(round_sem.at[k], n_adjacent)

    def table_part(step):
        at = pl.ds(pl.multiple_of(in_group(step) * 8, 128), plane * 8)
        return h_hbm.at[:, at, :], h.at[:, at, :]

    near = (1, GROUPS - 1)
    sources = [
        (x_hbm.at[0], x.at[0]),
        table_part(step_a),
        table_part(step_b),
        table_part(2),
        table_part(0),
        (x_hbm.at[1], x.at[1]),
        (h_hbm.at[:, pl.ds(x.shape[2], hz.shape[1]), pl.ds(0, hz.shape[1])], hz),
    ]
    loads = [
        pltpu.make_async_copy(src, dst, load_sem.at[k])
        for k, (src, dst) in enumerate(sources)
    ]
    for load in loads:
        load.start()

    def first(f, step):
        top = pl.multiple_of(in_group(step) * 8, 128)
        at = pl.ds(top, plane * 8)
        mid[...] = product((h[0, at], h[1, at]), (xs[f, 0], xs[f, 1]), ((1,), (1,)))

        @pl.loop(0, plane // 4)
        def _(g):
            for k in range(4):
                here = pl.ds(pl.multiple_of((g * 4 + k) * 8, 8), 8)
                v = swap_granules(mid[here, :128], mid[here, 128:])
                to_row[f, in_group(step) + g * 4 + k, :, :128] = v[0]
                to_row[f, in_group(step) + g * 4 + k, :, 128:] = v[1]

    def split(f):
        xs[f, 0], xs[f, 1] = halves(x[f])

    def z_copy(f, step):
        k = f * 3 + step - 1
        return pltpu.make_async_remote_copy(
            to_row.at[f, pl.ds(in_group(step), plane)], via.at[f, step - 1],
            z_send_sem.at[k], z_recv_sem.at[k],
            device_id=(in_group(step) + place, col), device_id_type=MESH,
        )

    def send_plane(f, step):
        source = in_group(GROUPS - step) + place if step else row

        def block(q):
            return via.at[f, step - 1, q] if step else to_row.at[f, row - place + q]

        @pl.loop(1, plane)
        def _(i):
            q = lax.rem(place + i, plane)
            pltpu.make_async_remote_copy(
                block(q), from_row.at[f, source], send_sem.at[f], recv_sem.at[f],
                device_id=(in_group(0) + q, col), device_id_type=MESH,
            ).start()

        from_row[f, source] = block(place)[...]

    def all_rows(f):
        count = GROUPS * (plane - 1)
        return pltpu.make_async_remote_copy(
            to_row.at[f, pl.ds(0, count)], from_row.at[f, pl.ds(0, count)],
            send_sem.at[f], recv_sem.at[f],
            device_id=(in_group(1) + place, col), device_id_type=MESH,
        )

    def second(f):
        lines = from_row[f].reshape(rows * 8, 256)
        modes = product((h[0], h[1]), halves(lines), ((1,), (0,)))
        for part in range(2):
            lanes = slice(128 * part, 128 * part + 128)
            to_col[f, part] = modes[:, lanes].reshape(cols, 64, 128)
            from_col[f, part, col] = to_col[f, part, col]

    def send_cols(f, part):
        for i in range(1, cols):
            peer = lax.rem(col + i, cols)
            pltpu.make_async_remote_copy(
                to_col.at[f, part, peer], from_col.at[f, part, col],
                send_sem.at[2 + 2 * f + part], recv_sem.at[2 + 2 * f + part],
                device_id=(row, peer), device_id_type=MESH,
            ).start()

    def all_cols(f, part):
        return pltpu.make_async_remote_copy(
            to_col.at[f, part, pl.ds(0, cols - 1)],
            from_col.at[f, part, pl.ds(0, cols - 1)],
            send_sem.at[2 + 2 * f + part], recv_sem.at[2 + 2 * f + part],
            device_id=(row, lax.rem(col + 1, cols)), device_id_type=MESH,
        )

    def third(f, part):
        @pl.loop(0, 8)
        def _(g):
            at = pl.ds(pl.multiple_of(g * 8, 8), 8)
            for j in range(2):
                v = swap_four([from_col[f, part, 4 * j + c, at] for c in range(4)])
                for k in range(4):
                    line[k, at, pl.ds(128 * j, 128)] = v[k]

        lines = line[...].reshape(256, 256)
        modes = product(halves(lines), (hz[0], hz[1]), ((1,), (0,)))
        out[f, 4 * part : 4 * part + 4] = modes.reshape(4, 64, 256)

    loads[0].wait()
    split(0)
    loads[1].wait()
    first(0, step_a)
    pl.semaphore_wait(barrier, n_lower + n_adjacent)
    answer()
    tell(0)

    @pl.when(group == 0)
    def _():
        pl.semaphore_wait(ready_sem.at[0], 1)

    z_copy(0, step_a).start()
    loads[2].wait()
    first(0, step_b)

    @pl.when(group != 2)
    def _():
        pl.semaphore_wait(ready_sem.at[1], 1)

    z_copy(0, step_b).start()
    for peer in (peer_a, peer_b):
        signal(ready_sem.at[2], peer)
    for k, step in ((3, 2), (4, 0)):
        loads[k].wait()
        first(0, step)
    hear(0)
    tell(1)
    loads[5].wait()
    split(1)
    first(1, step_a)
    hear(1)
    tell(2)
    pl.semaphore_wait(ready_sem.at[2], 2)
    z_copy(0, 2).start()
    z_copy(1, step_a).start()
    first(1, step_b)
    z_copy(1, step_b).start()
    first(1, 2)
    z_copy(1, 2).start()
    first(1, 0)
    hear(2)
    send_plane(0, 0)
    send_plane(1, 0)
    loads[6].wait()
    for f in range(2):
        for step in (*near, 2):
            z_copy(f, step).wait_recv()
            send_plane(f, step)
        all_rows(f).wait_recv()
        second(f)
        for part in range(2):
            send_cols(f, part)
    for f in range(2):
        for part in range(2):
            all_cols(f, part).wait_recv()
            third(f, part)
    for f in range(2):
        for step in (*near, 2):
            z_copy(f, step).wait_send()
        all_rows(f).wait_send()
        for part in range(2):
            all_cols(f, part).wait_send()


def divide(spectrum, sx, sy, sz, out, done, sems):
    row, col = lax.axis_index("row"), lax.axis_index("col")
    fields, share_x, share_y, nz = spectrum.shape
    lane = lax.broadcasted_iota(jnp.int32, (share_y, sy.shape[1]), 1)
    sub = lax.broadcasted_iota(jnp.int32, (share_y, sy.shape[1]), 0)
    mine = lane == col * share_y + sub
    part_y = jnp.sum(jnp.where(mine, sy[...], 0.0), axis=1, keepdims=True)
    lane_x = lax.broadcasted_iota(jnp.int32, sx.shape, 1)
    copies = []
    for k in range(share_x):
        mine = lane_x == row * share_x + k
        part_x = jnp.sum(jnp.where(mine, sx[...], 0.0), axis=1, keepdims=True)
        symbol = (part_x + part_y) + sz[...]
        for f in range(fields):
            done[f, k] = spectrum[f, k] / symbol
        if k % 2 == 1:
            two = pl.ds(k - 1, 2)
            copies.append(
                pltpu.make_async_copy(done.at[:, two], out.at[:, two], sems.at[k // 2])
            )
            copies[-1].start()
    for copy in copies:
        copy.wait()


def on_device(rows, cols, species, symbol_x, symbol_y, symbol_z):
    fields, nx, ny, nz = species.shape
    values = species.transpose(0, 2, 3, 1).reshape(fields, ny * nz, nx)
    table_z = np.pad(split_table(nz * cols), ((0, 0), (0, 0), (0, nx - nz * cols)))
    table = jnp.asarray(np.concatenate([split_table(nx), table_z], axis=1))
    share_x, share_y = nx // rows, ny * rows // cols
    in_hbm = pl.BlockSpec(memory_space=pltpu.HBM)
    in_vmem = pl.BlockSpec(memory_space=pltpu.VMEM)
    result = jax.ShapeDtypeStruct((fields, share_x, share_y, nz * cols), F32)
    spectrum = pl.pallas_call(
        functools.partial(kernel, rows, cols),
        out_shape=result,
        in_specs=[in_hbm] * 2,
        out_specs=in_vmem,
        scratch_shapes=[
            pltpu.VMEM(values.shape, F32),
            pltpu.VMEM((fields, 2, ny * nz, nx), BF16),
            pltpu.VMEM((2, nx, nx), BF16),
            pltpu.VMEM((2, nz * cols, nz * cols), BF16),
            pltpu.VMEM((nx // GROUPS, ny * nz), F32),
            pltpu.VMEM((fields, rows, 8, 256), F32),
            pltpu.VMEM((fields, GROUPS - 1, rows // GROUPS, 8, 256), F32),
            pltpu.VMEM((fields, rows, 8, 256), F32),
            pltpu.VMEM((fields, 2, cols, 64, 128), F32),
            pltpu.VMEM((fields, 2, cols, 64, 128), F32),
            pltpu.VMEM((4, 64, 256), F32),
            pltpu.SemaphoreType.DMA((7,)),
            pltpu.SemaphoreType.DMA((6,)),
            pltpu.SemaphoreType.DMA((6,)),
            pltpu.SemaphoreType.DMA((6,)),
            pltpu.SemaphoreType.DMA((6,)),
            pltpu.SemaphoreType.REGULAR((3,)),
            pltpu.SemaphoreType.REGULAR((3,)),
        ],
        compiler_params=pltpu.CompilerParams(
            collective_id=0, has_side_effects=True, vmem_limit_bytes=VMEM_LIMIT
        ),
    )(values, table)
    return pl.pallas_call(
        divide,
        out_shape=result,
        in_specs=[in_vmem] * 4,
        out_specs=in_hbm,
        scratch_shapes=[
            pltpu.VMEM(result.shape, F32),
            pltpu.SemaphoreType.DMA((share_x // 2,)),
        ],
        compiler_params=pltpu.CompilerParams(vmem_limit_bytes=8 * 2**20),
    )(spectrum, symbol_x[None], symbol_y[None], symbol_z[None])


def solution(mesh):
    in_specs = (P(None, None, "row", "col"), P(), P(), P())
    out_specs = P(None, "row", "col", None)
    return jax.shard_map(
        functools.partial(on_device, mesh.shape["row"], mesh.shape["col"]),
        mesh=mesh, in_specs=in_specs, out_specs=out_specs, check_vma=False,
    )
```

```python
import functools

import jax
import jax.numpy as jnp
import ml_dtypes
import numpy as np
from jax import lax
from jax.experimental import pallas as pl
from jax.experimental.pallas import tpu as pltpu
from jax.sharding import PartitionSpec as P

MESH = pl.DeviceIdType.MESH
F32 = jnp.float32
BF16 = jnp.bfloat16
GROUPS = 4
VMEM_LIMIT = 53500 * 2**10


def split_table(count):
    rank = np.arange(count, dtype=np.float64)
    angle = np.pi / (4 * count) * (2 * rank[:, None] + 1) * (2 * rank[None, :] + 1)
    table = (np.cos(angle) * np.sqrt(2.0 / count)).astype(np.float32)
    high = table.astype(ml_dtypes.bfloat16)
    low = (table - high.astype(np.float32)).astype(ml_dtypes.bfloat16)
    return np.stack([high, low])


def halves(values):
    high = values.astype(BF16)
    return high, (values - high.astype(F32)).astype(BF16)


def product(a, b, dims):
    dot = functools.partial(
        lax.dot_general, dimension_numbers=(dims, ((), ())), preferred_element_type=F32
    )
    return dot(a[0], b[0]) + dot(a[0], b[1]) + dot(a[1], b[0])


def swap_granules(v0, v1):
    sub = lax.broadcasted_iota(jnp.int32, (8, 128), 0)
    lane = lax.broadcasted_iota(jnp.int32, (8, 128), 1)
    upper = sub >= 4
    w0 = jnp.where(upper, pltpu.roll(v1, 4, 0), v0)
    w1 = jnp.where(upper, v1, pltpu.roll(v0, 4, 0))
    s1, g1 = (sub // 2) % 2, lane // 64
    s0, g0 = sub % 2, (lane // 32) % 2
    out = []
    for w in (w0, w1):
        u = pltpu.roll(w, 64, 1)
        w = jnp.where(
            s1 == g1, w, jnp.where(s1 == 0, pltpu.roll(u, 6, 0), pltpu.roll(u, 2, 0))
        )
        a, b = pltpu.roll(w, 32, 1), pltpu.roll(w, 96, 1)
        w = jnp.where(
            s0 == g0, w, jnp.where(s0 == 0, pltpu.roll(a, 7, 0), pltpu.roll(b, 1, 0))
        )
        out.append(w)
    return out


def swap_four(v):
    lane = lax.broadcasted_iota(jnp.int32, (8, 128), 1)
    g1, g0 = lane // 64 == 1, (lane // 32) % 2 == 1
    w = [None] * 4
    for k in range(2):
        a, b = v[k], v[k + 2]
        w[k] = jnp.where(g1, pltpu.roll(b, 64, 1), a)
        w[k + 2] = jnp.where(g1, b, pltpu.roll(a, 64, 1))
    o = [None] * 4
    for k in (0, 2):
        a, b = w[k], w[k + 1]
        o[k] = jnp.where(g0, pltpu.roll(b, 32, 1), a)
        o[k + 1] = jnp.where(g0, b, pltpu.roll(a, 96, 1))
    return o


def kernel(
    rows, cols, x_hbm, h_hbm, out, x, xs, h, hz, mid, to_row, via, from_row, to_col, from_col, line,
    load_sem, send_sem, recv_sem, z_send_sem, z_recv_sem, ready_sem, round_sem,
):
    row, col = lax.axis_index("row"), lax.axis_index("col")
    plane = rows // GROUPS
    group, place = row // plane, lax.rem(row, plane)

    def in_group(step):
        return lax.rem(group + step, GROUPS) * plane

    def signal(semaphore, peer):
        pl.semaphore_signal(semaphore, inc=1, device_id=peer, device_id_type=MESH)

    def in_plane(x_step, y_step):
        x = lax.rem(lax.rem(place, 4) + x_step, 4)
        y = lax.rem(place // 4 + y_step, 4)
        return row - place + 4 * y + x, col

    flip = lax.rem(group % 2 + group // 2, 2)
    step_a, step_b = 1 + 2 * flip, 3 - 2 * flip
    peer_a = (in_group(step_a) + place, col)
    peer_b = (in_group(step_b) + place, col)
    z_lo, core = col // 2, lax.rem(col, 2)
    x_at, y_at = lax.rem(place, 4), place // 4
    adjacent = [
        (x_at < 3, in_plane(1, 0)),
        (x_at == 0, in_plane(3, 0)),
        (y_at < 3, in_plane(0, 1)),
        (y_at == 0, in_plane(0, 3)),
        (core == 0, (row, col + 1 - 2 * core)),
    ]
    n_adjacent = len(adjacent) + 1 + z_lo * (3 - z_lo) // 2
    n_before = (x_at + 1) // 2 + (y_at + 1) // 2 + core + (z_lo + 3) // 4

    def signal_adjacent(semaphore, later, earlier):
        for is_later, peer in adjacent:
            if later and earlier:
                signal(semaphore, peer)
            else:

                @pl.when(is_later if later else jnp.logical_not(is_later))
                def _():
                    signal(semaphore, peer)

        if earlier:

            @pl.when(z_lo > 0)
            def _():
                signal(semaphore, (row, col - 2))

        if later:

            @pl.when(z_lo < 3)
            def _():
                signal(semaphore, (row, col + 2))

    barrier = pltpu.get_barrier_semaphore()
    n_lower = group % 2 + 2 * (group // 2) * (1 - group % 2)

    @pl.when(group == 0)
    def _():
        signal(barrier, peer_a)

    @pl.when(group != 2)
    def _():
        signal(barrier, peer_b)

    signal_adjacent(barrier, True, False)

    def answer():
        @pl.when(group == 1)
        def _():
            signal(ready_sem.at[0], peer_a)

        @pl.when(group >= 2)
        def _():
            signal(ready_sem.at[1], peer_a)

        @pl.when(group == 2)
        def _():
            signal(ready_sem.at[1], peer_b)

        signal_adjacent(round_sem.at[3], False, True)

    def tell(k):
        signal_adjacent(round_sem.at[k], True, True)

    def hear(k):
        pl.semaphore_wait(round_sem.at[k], n_adjacent)

    def table_part(step):
        at = pl.ds(pl.multiple_of(in_group(step) * 8, 128), plane * 8)
        return h_hbm.at[:, at, :], h.at[:, at, :]

    near = (1, GROUPS - 1)
    sources = [
        (x_hbm.at[0], x.at[0]),
        table_part(step_a),
        table_part(step_b),
        table_part(2),
        table_part(0),
        (x_hbm.at[1], x.at[1]),
        (h_hbm.at[:, pl.ds(x.shape[2], hz.shape[1]), pl.ds(0, hz.shape[1])], hz),
    ]
    loads = [
        pltpu.make_async_copy(src, dst, load_sem.at[k])
        for k, (src, dst) in enumerate(sources)
    ]
    for load in loads:
        load.start()

    def first(f, step):
        top = pl.multiple_of(in_group(step) * 8, 128)
        at = pl.ds(top, plane * 8)
        mid[...] = product((h[0, at], h[1, at]), (xs[f, 0], xs[f, 1]), ((1,), (1,)))

        for q in range(plane):
            v = swap_granules(mid[8 * q : 8 * q + 8, :128], mid[8 * q : 8 * q + 8, 128:])
            to_row[f, in_group(step) + q, :, :128] = v[0]
            to_row[f, in_group(step) + q, :, 128:] = v[1]

    def split(f):
        xs[f, 0], xs[f, 1] = halves(x[f])

    def z_copy(f, step):
        k = f * 3 + step - 1
        return pltpu.make_async_remote_copy(
            to_row.at[f, pl.ds(in_group(step), plane)], via.at[f, step - 1],
            z_send_sem.at[k], z_recv_sem.at[k],
            device_id=(in_group(step) + place, col), device_id_type=MESH,
        )

    def send_plane(f, step):
        source = in_group(GROUPS - step) + place if step else row

        def block(q):
            return via.at[f, step - 1, q] if step else to_row.at[f, row - place + q]

        @pl.loop(1, plane)
        def _(i):
            q = lax.rem(place + i, plane)
            pltpu.make_async_remote_copy(
                block(q), from_row.at[f, source], send_sem.at[f], recv_sem.at[f],
                device_id=(in_group(0) + q, col), device_id_type=MESH,
            ).start()

        from_row[f, source] = block(place)[...]

    def all_rows(f):
        count = GROUPS * (plane - 1)
        return pltpu.make_async_remote_copy(
            to_row.at[f, pl.ds(0, count)], from_row.at[f, pl.ds(0, count)],
            send_sem.at[f], recv_sem.at[f],
            device_id=(in_group(1) + place, col), device_id_type=MESH,
        )

    def second(f):
        lines = from_row[f].reshape(rows * 8, 256)
        modes = product((h[0], h[1]), halves(lines), ((1,), (0,)))
        for part in range(2):
            lanes = slice(128 * part, 128 * part + 128)
            to_col[f, part] = modes[:, lanes].reshape(cols, 64, 128)
            from_col[f, part, col] = to_col[f, part, col]

    def send_cols(f, part):
        for i in range(1, cols):
            peer = lax.rem(col + i, cols)
            pltpu.make_async_remote_copy(
                to_col.at[f, part, peer], from_col.at[f, part, col],
                send_sem.at[2 + 2 * f + part], recv_sem.at[2 + 2 * f + part],
                device_id=(row, peer), device_id_type=MESH,
            ).start()

    def all_cols(f, part):
        return pltpu.make_async_remote_copy(
            to_col.at[f, part, pl.ds(0, cols - 1)],
            from_col.at[f, part, pl.ds(0, cols - 1)],
            send_sem.at[2 + 2 * f + part], recv_sem.at[2 + 2 * f + part],
            device_id=(row, lax.rem(col + 1, cols)), device_id_type=MESH,
        )

    def third(f, part):
        for g in range(8):
            at = slice(8 * g, 8 * g + 8)
            for j in range(2):
                v = swap_four([from_col[f, part, 4 * j + c, at] for c in range(4)])
                for k in range(4):
                    line[k, at, 128 * j : 128 * j + 128] = v[k]

        lines = line[...].reshape(256, 256)
        modes = product(halves(lines), (hz[0], hz[1]), ((1,), (0,)))
        out[f, 4 * part : 4 * part + 4] = modes.reshape(4, 64, 256)

    @pl.when(jnp.logical_and(group != 2, n_lower + n_before > 0))
    def _():
        pl.semaphore_wait(barrier, n_lower + n_before)
        answer()

    loads[0].wait()
    split(0)
    loads[1].wait()
    first(0, step_a)

    @pl.when(group == 2)
    def _():
        pl.semaphore_wait(barrier, n_lower + n_before)
        answer()

    @pl.when(group == 0)
    def _():
        pl.semaphore_wait(ready_sem.at[0], 1)

    z_copy(0, step_a).start()
    loads[2].wait()
    first(0, step_b)

    @pl.when(group != 2)
    def _():
        pl.semaphore_wait(ready_sem.at[1], 1)

    z_copy(0, step_b).start()
    for peer in (peer_a, peer_b):
        signal(ready_sem.at[2], peer)

    @pl.when(n_adjacent > n_before)
    def _():
        pl.semaphore_wait(round_sem.at[3], n_adjacent - n_before)

    tell(0)
    for k, step in ((3, 2), (4, 0)):
        loads[k].wait()
        first(0, step)
    hear(0)
    tell(1)
    loads[5].wait()
    split(1)
    first(1, step_a)
    hear(1)
    tell(2)
    pl.semaphore_wait(ready_sem.at[2], 2)
    z_copy(0, 2).start()
    z_copy(1, step_a).start()
    first(1, step_b)
    z_copy(1, step_b).start()
    first(1, 2)
    z_copy(1, 2).start()
    first(1, 0)
    hear(2)
    send_plane(0, 0)
    send_plane(1, 0)
    loads[6].wait()
    for f in range(2):
        for step in (*near, 2):
            z_copy(f, step).wait_recv()
            send_plane(f, step)
        all_rows(f).wait_recv()
        second(f)
        for part in range(2):
            send_cols(f, part)
    for f in range(2):
        for part in range(2):
            all_cols(f, part).wait_recv()
            third(f, part)
    for f in range(2):
        for step in (*near, 2):
            z_copy(f, step).wait_send()
        all_rows(f).wait_send()
        for part in range(2):
            all_cols(f, part).wait_send()


def divide(spectrum, sx, sy, sz, out, done, sems):
    row, col = lax.axis_index("row"), lax.axis_index("col")
    fields, share_x, share_y, nz = spectrum.shape
    lane = lax.broadcasted_iota(jnp.int32, (share_y, sy.shape[1]), 1)
    sub = lax.broadcasted_iota(jnp.int32, (share_y, sy.shape[1]), 0)
    mine = lane == col * share_y + sub
    part_y = jnp.sum(jnp.where(mine, sy[...], 0.0), axis=1, keepdims=True)
    lane_x = lax.broadcasted_iota(jnp.int32, sx.shape, 1)
    copies = []
    for k in range(share_x):
        mine = lane_x == row * share_x + k
        part_x = jnp.sum(jnp.where(mine, sx[...], 0.0), axis=1, keepdims=True)
        symbol = (part_x + part_y) + sz[...]
        for f in range(fields):
            done[f, k] = spectrum[f, k] / symbol
        if k % 2 == 1:
            two = pl.ds(k - 1, 2)
            copies.append(
                pltpu.make_async_copy(done.at[:, two], out.at[:, two], sems.at[k // 2])
            )
            copies[-1].start()
    for copy in copies:
        copy.wait()


def on_device(rows, cols, species, symbol_x, symbol_y, symbol_z):
    fields, nx, ny, nz = species.shape
    values = species.transpose(0, 2, 3, 1).reshape(fields, ny * nz, nx)
    table_z = np.pad(split_table(nz * cols), ((0, 0), (0, 0), (0, nx - nz * cols)))
    table = jnp.asarray(np.concatenate([split_table(nx), table_z], axis=1))
    share_x, share_y = nx // rows, ny * rows // cols
    in_hbm = pl.BlockSpec(memory_space=pltpu.HBM)
    in_vmem = pl.BlockSpec(memory_space=pltpu.VMEM)
    result = jax.ShapeDtypeStruct((fields, share_x, share_y, nz * cols), F32)
    spectrum = pl.pallas_call(
        functools.partial(kernel, rows, cols),
        out_shape=result,
        in_specs=[in_hbm] * 2,
        out_specs=in_vmem,
        scratch_shapes=[
            pltpu.VMEM(values.shape, F32),
            pltpu.VMEM((fields, 2, ny * nz, nx), BF16),
            pltpu.VMEM((2, nx, nx), BF16),
            pltpu.VMEM((2, nz * cols, nz * cols), BF16),
            pltpu.VMEM((nx // GROUPS, ny * nz), F32),
            pltpu.VMEM((fields, rows, 8, 256), F32),
            pltpu.VMEM((fields, GROUPS - 1, rows // GROUPS, 8, 256), F32),
            pltpu.VMEM((fields, rows, 8, 256), F32),
            pltpu.VMEM((fields, 2, cols, 64, 128), F32),
            pltpu.VMEM((fields, 2, cols, 64, 128), F32),
            pltpu.VMEM((4, 64, 256), F32),
            pltpu.SemaphoreType.DMA((7,)),
            pltpu.SemaphoreType.DMA((6,)),
            pltpu.SemaphoreType.DMA((6,)),
            pltpu.SemaphoreType.DMA((6,)),
            pltpu.SemaphoreType.DMA((6,)),
            pltpu.SemaphoreType.REGULAR((3,)),
            pltpu.SemaphoreType.REGULAR((4,)),
        ],
        compiler_params=pltpu.CompilerParams(
            collective_id=0, has_side_effects=True, vmem_limit_bytes=VMEM_LIMIT
        ),
    )(values, table)
    return pl.pallas_call(
        divide,
        out_shape=result,
        in_specs=[in_vmem] * 4,
        out_specs=in_hbm,
        scratch_shapes=[
            pltpu.VMEM(result.shape, F32),
            pltpu.SemaphoreType.DMA((share_x // 2,)),
        ],
        compiler_params=pltpu.CompilerParams(vmem_limit_bytes=8 * 2**20),
    )(spectrum, symbol_x[None], symbol_y[None], symbol_z[None])


def solution(mesh):
    in_specs = (P(None, None, "row", "col"), P(), P(), P())
    out_specs = P(None, "row", "col", None)
    return jax.shard_map(
        functools.partial(on_device, mesh.shape["row"], mesh.shape["col"]),
        mesh=mesh, in_specs=in_specs, out_specs=out_specs, check_vma=False,
    )
```

```python
import functools

import jax
import jax.numpy as jnp
import ml_dtypes
import numpy as np
from jax import lax
from jax.experimental import pallas as pl
from jax.experimental.pallas import tpu as pltpu
from jax.sharding import PartitionSpec as P

MESH = pl.DeviceIdType.MESH
F32 = jnp.float32
BF16 = jnp.bfloat16
GROUPS = 4
NB = 4
VMEM_LIMIT = 53500 * 2**10


def split_table(count):
    rank = np.arange(count, dtype=np.float64)
    angle = np.pi / (4 * count) * (2 * rank[:, None] + 1) * (2 * rank[None, :] + 1)
    table = (np.cos(angle) * np.sqrt(2.0 / count)).astype(np.float32)
    high = table.astype(ml_dtypes.bfloat16)
    low = (table - high.astype(np.float32)).astype(ml_dtypes.bfloat16)
    return np.stack([high, low])


def halves(values):
    high = values.astype(BF16)
    return high, (values - high.astype(F32)).astype(BF16)


def product(a, b, dims):
    dot = functools.partial(
        lax.dot_general, dimension_numbers=(dims, ((), ())), preferred_element_type=F32
    )
    return dot(a[0], b[0]) + dot(a[0], b[1]) + dot(a[1], b[0])


def swap_granules(v0, v1):
    sub = lax.broadcasted_iota(jnp.int32, (8, 128), 0)
    lane = lax.broadcasted_iota(jnp.int32, (8, 128), 1)
    upper = sub >= 4
    w0 = jnp.where(upper, pltpu.roll(v1, 4, 0), v0)
    w1 = jnp.where(upper, v1, pltpu.roll(v0, 4, 0))
    s1, g1 = (sub // 2) % 2, lane // 64
    s0, g0 = sub % 2, (lane // 32) % 2
    out = []
    for w in (w0, w1):
        u = pltpu.roll(w, 64, 1)
        w = jnp.where(
            s1 == g1, w, jnp.where(s1 == 0, pltpu.roll(u, 6, 0), pltpu.roll(u, 2, 0))
        )
        a, b = pltpu.roll(w, 32, 1), pltpu.roll(w, 96, 1)
        w = jnp.where(
            s0 == g0, w, jnp.where(s0 == 0, pltpu.roll(a, 7, 0), pltpu.roll(b, 1, 0))
        )
        out.append(w)
    return out


def swap_four(v):
    lane = lax.broadcasted_iota(jnp.int32, (8, 128), 1)
    g1, g0 = lane // 64 == 1, (lane // 32) % 2 == 1
    w = [None] * 4
    for k in range(2):
        a, b = v[k], v[k + 2]
        w[k] = jnp.where(g1, pltpu.roll(b, 64, 1), a)
        w[k + 2] = jnp.where(g1, b, pltpu.roll(a, 64, 1))
    o = [None] * 4
    for k in (0, 2):
        a, b = w[k], w[k + 1]
        o[k] = jnp.where(g0, pltpu.roll(b, 32, 1), a)
        o[k + 1] = jnp.where(g0, b, pltpu.roll(a, 96, 1))
    return o


def kernel(
    rows, cols, x_hbm, h_hbm, out, x, xs, h, hz, mid, to_row, via, relay, from_row, to_col, from_col, line,
    load_sem, send_sem, recv_sem, z_send_sem, z_recv_sem, relay_sem, on_sem,
    ready_sem, round_sem,
):
    row, col = lax.axis_index("row"), lax.axis_index("col")
    plane = rows // GROUPS
    group, place = row // plane, lax.rem(row, plane)

    def in_group(step):
        return lax.rem(group + step, GROUPS) * plane

    def signal(semaphore, peer):
        pl.semaphore_signal(semaphore, inc=1, device_id=peer, device_id_type=MESH)

    def in_plane(x_step, y_step):
        x = lax.rem(lax.rem(place, 4) + x_step, 4)
        y = lax.rem(place // 4 + y_step, 4)
        return row - place + 4 * y + x, col

    flip = lax.rem(group % 2 + group // 2, 2)
    step_a, step_b = 1 + 2 * flip, 3 - 2 * flip
    peer_a = (in_group(step_a) + place, col)
    peer_b = (in_group(step_b) + place, col)
    z_lo, core = col // 2, lax.rem(col, 2)
    x_at, y_at = lax.rem(place, 4), place // 4
    adjacent = [
        (x_at < 3, in_plane(1, 0)),
        (x_at == 0, in_plane(3, 0)),
        (y_at < 3, in_plane(0, 1)),
        (y_at == 0, in_plane(0, 3)),
        (core == 0, (row, col + 1 - 2 * core)),
    ]
    n_adjacent = len(adjacent) + 1 + z_lo * (3 - z_lo) // 2
    n_before = (x_at + 1) // 2 + (y_at + 1) // 2 + core + (z_lo + 3) // 4

    def signal_adjacent(semaphore, later, earlier):
        for is_later, peer in adjacent:
            if later and earlier:
                signal(semaphore, peer)
            else:

                @pl.when(is_later if later else jnp.logical_not(is_later))
                def _():
                    signal(semaphore, peer)

        if earlier:

            @pl.when(z_lo > 0)
            def _():
                signal(semaphore, (row, col - 2))

        if later:

            @pl.when(z_lo < 3)
            def _():
                signal(semaphore, (row, col + 2))

    barrier = pltpu.get_barrier_semaphore()
    n_lower = group % 2 + 2 * (group // 2) * (1 - group % 2)

    @pl.when(group == 0)
    def _():
        signal(barrier, peer_a)

    @pl.when(group != 2)
    def _():
        signal(barrier, peer_b)

    signal_adjacent(barrier, True, False)

    def answer():
        @pl.when(group == 1)
        def _():
            signal(ready_sem.at[0], peer_a)

        @pl.when(group >= 2)
        def _():
            signal(ready_sem.at[1], peer_a)

        @pl.when(group == 2)
        def _():
            signal(ready_sem.at[1], peer_b)

        signal_adjacent(round_sem.at[3], False, True)

    def tell(k):
        signal_adjacent(round_sem.at[k], True, True)

    def hear(k):
        pl.semaphore_wait(round_sem.at[k], n_adjacent)

    def table_part(step):
        at = pl.ds(pl.multiple_of(in_group(step) * 8, 128), plane * 8)
        return h_hbm.at[:, at, :], h.at[:, at, :]

    near = (1, GROUPS - 1)
    sources = [
        (x_hbm.at[0], x.at[0]),
        table_part(step_a),
        table_part(step_b),
        table_part(2),
        table_part(0),
        (x_hbm.at[1], x.at[1]),
        (h_hbm.at[:, pl.ds(x.shape[2], hz.shape[1]), pl.ds(0, hz.shape[1])], hz),
    ]
    loads = [
        pltpu.make_async_copy(src, dst, load_sem.at[k])
        for k, (src, dst) in enumerate(sources)
    ]
    for load in loads:
        load.start()

    def first(f, step):
        top = pl.multiple_of(in_group(step) * 8, 128)
        at = pl.ds(top, plane * 8)
        mid[...] = product((h[0, at], h[1, at]), (xs[f, 0], xs[f, 1]), ((1,), (1,)))

        for q in range(plane):
            v = swap_granules(mid[8 * q : 8 * q + 8, :128], mid[8 * q : 8 * q + 8, 128:])
            to_row[f, in_group(step) + q, :, :128] = v[0]
            to_row[f, in_group(step) + q, :, 128:] = v[1]

    def split(f):
        xs[f, 0], xs[f, 1] = halves(x[f])

    def z_copy(f, step):
        k = f * 3 + step - 1
        return pltpu.make_async_remote_copy(
            to_row.at[f, pl.ds(in_group(step), plane)], via.at[f, step - 1],
            z_send_sem.at[k], z_recv_sem.at[k],
            device_id=(in_group(step) + place, col), device_id_type=MESH,
        )

    def far_copy(f):
        return pltpu.make_async_remote_copy(
            to_row.at[f, pl.ds(in_group(2) + NB, plane - NB)], via.at[f, 1, pl.ds(NB, plane - NB)],
            z_send_sem.at[f * 3 + 1], z_recv_sem.at[f * 3 + 1],
            device_id=(in_group(2) + place, col), device_id_type=MESH,
        )

    def relay_copy(f, side):
        return pltpu.make_async_remote_copy(
            to_row.at[f, pl.ds(in_group(2), NB)], relay.at[f, side],
            z_send_sem.at[f * 3 + 1], relay_sem.at[2 * f + side],
            device_id=peer_b, device_id_type=MESH,
        )

    def on_copy(f, side):
        return pltpu.make_async_remote_copy(
            relay.at[f, side], via.at[f, 1, pl.ds(0, NB)],
            on_sem.at[2 * f + side], z_recv_sem.at[f * 3 + 1],
            device_id=peer_a if side else peer_b, device_id_type=MESH,
        )

    odd = lax.rem(group, 2) == 1

    def start_far(f):
        @pl.when(odd)
        def _():
            far_copy(f).start()

        @pl.when(jnp.logical_not(odd))
        def _():
            z_copy(f, 2).start()

    def start_relay(f):
        @pl.when(odd)
        def _():
            relay_copy(f, group // 2).start()

    def send_on(f):
        @pl.when(group == 2)
        def _():
            for side in range(2):
                relay_copy(f, side).wait_recv()
                on_copy(f, side).start()

    def send_plane(f, step):
        source = in_group(GROUPS - step) + place if step else row

        def block(q):
            return via.at[f, step - 1, q] if step else to_row.at[f, row - place + q]

        @pl.loop(1, plane)
        def _(i):
            q = lax.rem(place + i, plane)
            pltpu.make_async_remote_copy(
                block(q), from_row.at[f, source], send_sem.at[f], recv_sem.at[f],
                device_id=(in_group(0) + q, col), device_id_type=MESH,
            ).start()

        from_row[f, source] = block(place)[...]

    def all_rows(f):
        count = GROUPS * (plane - 1)
        return pltpu.make_async_remote_copy(
            to_row.at[f, pl.ds(0, count)], from_row.at[f, pl.ds(0, count)],
            send_sem.at[f], recv_sem.at[f],
            device_id=(in_group(1) + place, col), device_id_type=MESH,
        )

    def second(f):
        lines = from_row[f].reshape(rows * 8, 256)
        modes = product((h[0], h[1]), halves(lines), ((1,), (0,)))
        for part in range(2):
            lanes = slice(128 * part, 128 * part + 128)
            to_col[f, part] = modes[:, lanes].reshape(cols, 64, 128)
            from_col[f, part, col] = to_col[f, part, col]

    def send_cols(f, part):
        for i in range(1, cols):
            peer = lax.rem(col + i, cols)
            pltpu.make_async_remote_copy(
                to_col.at[f, part, peer], from_col.at[f, part, col],
                send_sem.at[2 + 2 * f + part], recv_sem.at[2 + 2 * f + part],
                device_id=(row, peer), device_id_type=MESH,
            ).start()

    def all_cols(f, part):
        return pltpu.make_async_remote_copy(
            to_col.at[f, part, pl.ds(0, cols - 1)],
            from_col.at[f, part, pl.ds(0, cols - 1)],
            send_sem.at[2 + 2 * f + part], recv_sem.at[2 + 2 * f + part],
            device_id=(row, lax.rem(col + 1, cols)), device_id_type=MESH,
        )

    def third(f, part):
        for g in range(8):
            at = slice(8 * g, 8 * g + 8)
            for j in range(2):
                v = swap_four([from_col[f, part, 4 * j + c, at] for c in range(4)])
                for k in range(4):
                    line[k, at, 128 * j : 128 * j + 128] = v[k]

        lines = line[...].reshape(256, 256)
        modes = product(halves(lines), (hz[0], hz[1]), ((1,), (0,)))
        out[f, 4 * part : 4 * part + 4] = modes.reshape(4, 64, 256)

    @pl.when(jnp.logical_and(group != 2, n_lower + n_before > 0))
    def _():
        pl.semaphore_wait(barrier, n_lower + n_before)
        answer()

    loads[0].wait()
    split(0)
    loads[1].wait()
    first(0, step_a)

    @pl.when(group == 2)
    def _():
        pl.semaphore_wait(barrier, n_lower + n_before)
        answer()

    @pl.when(group == 0)
    def _():
        pl.semaphore_wait(ready_sem.at[0], 1)

    z_copy(0, step_a).start()
    loads[2].wait()
    first(0, step_b)
    loads[3].wait()
    first(0, 2)

    @pl.when(group != 2)
    def _():
        pl.semaphore_wait(ready_sem.at[1], 1)

    start_relay(0)
    z_copy(0, step_b).start()
    for peer in (peer_a, peer_b):
        signal(ready_sem.at[2], peer)

    @pl.when(n_adjacent > n_before)
    def _():
        pl.semaphore_wait(round_sem.at[3], n_adjacent - n_before)

    tell(0)
    loads[4].wait()
    first(0, 0)
    hear(0)
    tell(1)
    loads[5].wait()
    split(1)
    first(1, step_a)
    hear(1)
    tell(2)
    pl.semaphore_wait(ready_sem.at[2], 2)
    start_far(0)
    send_on(0)
    z_copy(1, step_a).start()
    first(1, step_b)
    first(1, 2)
    start_relay(1)
    z_copy(1, step_b).start()
    start_far(1)
    first(1, 0)
    hear(2)
    send_plane(0, 0)
    send_plane(1, 0)
    loads[6].wait()
    for f in range(2):
        for step in (*near, 2):
            z_copy(f, step).wait_recv()
            send_plane(f, step)
        if f == 0:
            send_on(1)
        all_rows(f).wait_recv()
        second(f)
        for part in range(2):
            send_cols(f, part)
    for f in range(2):
        for part in range(2):
            all_cols(f, part).wait_recv()
            third(f, part)
    for f in range(2):
        for step in (*near, 2):
            z_copy(f, step).wait_send()
        all_rows(f).wait_send()
        for part in range(2):
            all_cols(f, part).wait_send()

        @pl.when(group == 2)
        def _():
            for side in range(2):
                on_copy(f, side).wait_send()


def divide(spectrum, sx, sy, sz, out, done, sems):
    row, col = lax.axis_index("row"), lax.axis_index("col")
    fields, share_x, share_y, nz = spectrum.shape
    lane = lax.broadcasted_iota(jnp.int32, (share_y, sy.shape[1]), 1)
    sub = lax.broadcasted_iota(jnp.int32, (share_y, sy.shape[1]), 0)
    mine = lane == col * share_y + sub
    part_y = jnp.sum(jnp.where(mine, sy[...], 0.0), axis=1, keepdims=True)
    lane_x = lax.broadcasted_iota(jnp.int32, sx.shape, 1)
    copies = []
    for k in range(share_x):
        mine = lane_x == row * share_x + k
        part_x = jnp.sum(jnp.where(mine, sx[...], 0.0), axis=1, keepdims=True)
        symbol = (part_x + part_y) + sz[...]
        for f in range(fields):
            done[f, k] = spectrum[f, k] / symbol
        if k % 2 == 1:
            two = pl.ds(k - 1, 2)
            copies.append(
                pltpu.make_async_copy(done.at[:, two], out.at[:, two], sems.at[k // 2])
            )
            copies[-1].start()
    for copy in copies:
        copy.wait()


def on_device(rows, cols, species, symbol_x, symbol_y, symbol_z):
    fields, nx, ny, nz = species.shape
    values = species.transpose(0, 2, 3, 1).reshape(fields, ny * nz, nx)
    table_z = np.pad(split_table(nz * cols), ((0, 0), (0, 0), (0, nx - nz * cols)))
    table = jnp.asarray(np.concatenate([split_table(nx), table_z], axis=1))
    share_x, share_y = nx // rows, ny * rows // cols
    in_hbm = pl.BlockSpec(memory_space=pltpu.HBM)
    in_vmem = pl.BlockSpec(memory_space=pltpu.VMEM)
    result = jax.ShapeDtypeStruct((fields, share_x, share_y, nz * cols), F32)
    spectrum = pl.pallas_call(
        functools.partial(kernel, rows, cols),
        out_shape=result,
        in_specs=[in_hbm] * 2,
        out_specs=in_vmem,
        scratch_shapes=[
            pltpu.VMEM(values.shape, F32),
            pltpu.VMEM((fields, 2, ny * nz, nx), BF16),
            pltpu.VMEM((2, nx, nx), BF16),
            pltpu.VMEM((2, nz * cols, nz * cols), BF16),
            pltpu.VMEM((nx // GROUPS, ny * nz), F32),
            pltpu.VMEM((fields, rows, 8, 256), F32),
            pltpu.VMEM((fields, GROUPS - 1, rows // GROUPS, 8, 256), F32),
            pltpu.VMEM((fields, 2, NB, 8, 256), F32),
            pltpu.VMEM((fields, rows, 8, 256), F32),
            pltpu.VMEM((fields, 2, cols, 64, 128), F32),
            pltpu.VMEM((fields, 2, cols, 64, 128), F32),
            pltpu.VMEM((4, 64, 256), F32),
            pltpu.SemaphoreType.DMA((7,)),
            pltpu.SemaphoreType.DMA((6,)),
            pltpu.SemaphoreType.DMA((6,)),
            pltpu.SemaphoreType.DMA((6,)),
            pltpu.SemaphoreType.DMA((6,)),
            pltpu.SemaphoreType.DMA((4,)),
            pltpu.SemaphoreType.DMA((4,)),
            pltpu.SemaphoreType.REGULAR((3,)),
            pltpu.SemaphoreType.REGULAR((4,)),
        ],
        compiler_params=pltpu.CompilerParams(
            collective_id=0, has_side_effects=True, vmem_limit_bytes=VMEM_LIMIT
        ),
    )(values, table)
    return pl.pallas_call(
        divide,
        out_shape=result,
        in_specs=[in_vmem] * 4,
        out_specs=in_hbm,
        scratch_shapes=[
            pltpu.VMEM(result.shape, F32),
            pltpu.SemaphoreType.DMA((share_x // 2,)),
        ],
        compiler_params=pltpu.CompilerParams(vmem_limit_bytes=8 * 2**20),
    )(spectrum, symbol_x[None], symbol_y[None], symbol_z[None])


def solution(mesh):
    in_specs = (P(None, None, "row", "col"), P(), P(), P())
    out_specs = P(None, "row", "col", None)
    return jax.shard_map(
        functools.partial(on_device, mesh.shape["row"], mesh.shape["col"]),
        mesh=mesh, in_specs=in_specs, out_specs=out_specs, check_vma=False,
    )
```

```python
import functools

import jax
import jax.numpy as jnp
import ml_dtypes
import numpy as np
from jax import lax
from jax.experimental import pallas as pl
from jax.experimental.pallas import tpu as pltpu
from jax.sharding import PartitionSpec as P

MESH = pl.DeviceIdType.MESH
F32 = jnp.float32
BF16 = jnp.bfloat16
GROUPS = 4
NB = 4
VMEM_LIMIT = 53500 * 2**10


def split_table(count):
    rank = np.arange(count, dtype=np.float64)
    angle = np.pi / (4 * count) * (2 * rank[:, None] + 1) * (2 * rank[None, :] + 1)
    table = (np.cos(angle) * np.sqrt(2.0 / count)).astype(np.float32)
    high = table.astype(ml_dtypes.bfloat16)
    low = (table - high.astype(np.float32)).astype(ml_dtypes.bfloat16)
    return np.stack([high, low])


def halves(values):
    high = values.astype(BF16)
    return high, (values - high.astype(F32)).astype(BF16)


def product(a, b, dims):
    dot = functools.partial(
        lax.dot_general, dimension_numbers=(dims, ((), ())), preferred_element_type=F32
    )
    return dot(a[0], b[0]) + dot(a[0], b[1]) + dot(a[1], b[0])


def swap_granules(v0, v1):
    sub = lax.broadcasted_iota(jnp.int32, (8, 128), 0)
    lane = lax.broadcasted_iota(jnp.int32, (8, 128), 1)
    upper = sub >= 4
    w0 = jnp.where(upper, pltpu.roll(v1, 4, 0), v0)
    w1 = jnp.where(upper, v1, pltpu.roll(v0, 4, 0))
    s1, g1 = (sub // 2) % 2, lane // 64
    s0, g0 = sub % 2, (lane // 32) % 2
    out = []
    for w in (w0, w1):
        u = pltpu.roll(w, 64, 1)
        w = jnp.where(
            s1 == g1, w, jnp.where(s1 == 0, pltpu.roll(u, 6, 0), pltpu.roll(u, 2, 0))
        )
        a, b = pltpu.roll(w, 32, 1), pltpu.roll(w, 96, 1)
        w = jnp.where(
            s0 == g0, w, jnp.where(s0 == 0, pltpu.roll(a, 7, 0), pltpu.roll(b, 1, 0))
        )
        out.append(w)
    return out


def swap_four(v):
    lane = lax.broadcasted_iota(jnp.int32, (8, 128), 1)
    g1, g0 = lane // 64 == 1, (lane // 32) % 2 == 1
    w = [None] * 4
    for k in range(2):
        a, b = v[k], v[k + 2]
        w[k] = jnp.where(g1, pltpu.roll(b, 64, 1), a)
        w[k + 2] = jnp.where(g1, b, pltpu.roll(a, 64, 1))
    o = [None] * 4
    for k in (0, 2):
        a, b = w[k], w[k + 1]
        o[k] = jnp.where(g0, pltpu.roll(b, 32, 1), a)
        o[k + 1] = jnp.where(g0, b, pltpu.roll(a, 96, 1))
    return o


def kernel(
    rows, cols, x_hbm, h_hbm, out, x, xs, h, hz, mid, to_row, via, relay, from_row, to_col, from_col, line,
    load_sem, send_sem, recv_sem, z_send_sem, z_recv_sem, relay_sem, on_sem,
    ready_sem, round_sem,
):
    row, col = lax.axis_index("row"), lax.axis_index("col")
    plane = rows // GROUPS
    group, place = row // plane, lax.rem(row, plane)

    def in_group(step):
        return lax.rem(group + step, GROUPS) * plane

    def signal(semaphore, peer):
        pl.semaphore_signal(semaphore, inc=1, device_id=peer, device_id_type=MESH)

    def in_plane(x_step, y_step):
        x = lax.rem(lax.rem(place, 4) + x_step, 4)
        y = lax.rem(place // 4 + y_step, 4)
        return row - place + 4 * y + x, col

    flip = lax.rem(group % 2 + group // 2, 2)
    step_a, step_b = 1 + 2 * flip, 3 - 2 * flip
    peer_a = (in_group(step_a) + place, col)
    peer_b = (in_group(step_b) + place, col)
    z_lo, core = col // 2, lax.rem(col, 2)
    x_at, y_at = lax.rem(place, 4), place // 4
    adjacent = [
        (x_at < 3, in_plane(1, 0)),
        (x_at == 0, in_plane(3, 0)),
        (y_at < 3, in_plane(0, 1)),
        (y_at == 0, in_plane(0, 3)),
        (core == 0, (row, col + 1 - 2 * core)),
    ]
    n_adjacent = len(adjacent) + 1 + z_lo * (3 - z_lo) // 2
    n_before = (x_at + 1) // 2 + (y_at + 1) // 2 + core + (z_lo + 3) // 4

    def signal_adjacent(semaphore, later, earlier):
        for is_later, peer in adjacent:
            if later and earlier:
                signal(semaphore, peer)
            else:

                @pl.when(is_later if later else jnp.logical_not(is_later))
                def _():
                    signal(semaphore, peer)

        if earlier:

            @pl.when(z_lo > 0)
            def _():
                signal(semaphore, (row, col - 2))

        if later:

            @pl.when(z_lo < 3)
            def _():
                signal(semaphore, (row, col + 2))

    barrier = pltpu.get_barrier_semaphore()
    n_lower = group % 2 + 2 * (group // 2) * (1 - group % 2)

    @pl.when(group == 0)
    def _():
        signal(barrier, peer_a)

    @pl.when(group != 2)
    def _():
        signal(barrier, peer_b)

    signal_adjacent(barrier, True, False)

    def answer():
        @pl.when(group == 1)
        def _():
            signal(ready_sem.at[0], peer_a)

        @pl.when(group >= 2)
        def _():
            signal(ready_sem.at[1], peer_a)

        @pl.when(group == 2)
        def _():
            signal(ready_sem.at[1], peer_b)

        signal_adjacent(round_sem.at[3], False, True)

    def tell(k):
        signal_adjacent(round_sem.at[k], True, True)

    def hear(k):
        pl.semaphore_wait(round_sem.at[k], n_adjacent)

    def table_part(step):
        at = pl.ds(pl.multiple_of(in_group(step) * 8, 128), plane * 8)
        return h_hbm.at[:, at, :], h.at[:, at, :]

    near = (1, GROUPS - 1)
    sources = [
        (x_hbm.at[0], x.at[0]),
        table_part(step_a),
        table_part(step_b),
        table_part(2),
        table_part(0),
        (x_hbm.at[1], x.at[1]),
        (h_hbm.at[:, pl.ds(x.shape[2], hz.shape[1]), pl.ds(0, hz.shape[1])], hz),
    ]
    loads = [
        pltpu.make_async_copy(src, dst, load_sem.at[k])
        for k, (src, dst) in enumerate(sources)
    ]
    for load in loads[:2]:
        load.start()

    def first(f, step):
        top = pl.multiple_of(in_group(step) * 8, 128)
        at = pl.ds(top, plane * 8)
        mid[...] = product((h[0, at], h[1, at]), (xs[f, 0], xs[f, 1]), ((1,), (1,)))

        for q in range(plane):
            v = swap_granules(mid[8 * q : 8 * q + 8, :128], mid[8 * q : 8 * q + 8, 128:])
            to_row[f, in_group(step) + q, :, :128] = v[0]
            to_row[f, in_group(step) + q, :, 128:] = v[1]

    def split(f):
        xs[f, 0], xs[f, 1] = halves(x[f])

    def z_copy(f, step):
        k = f * 3 + step - 1
        return pltpu.make_async_remote_copy(
            to_row.at[f, pl.ds(in_group(step), plane)], via.at[f, step - 1],
            z_send_sem.at[k], z_recv_sem.at[k],
            device_id=(in_group(step) + place, col), device_id_type=MESH,
        )

    def far_copy(f):
        return pltpu.make_async_remote_copy(
            to_row.at[f, pl.ds(in_group(2) + NB, plane - NB)], via.at[f, 1, pl.ds(NB, plane - NB)],
            z_send_sem.at[f * 3 + 1], z_recv_sem.at[f * 3 + 1],
            device_id=(in_group(2) + place, col), device_id_type=MESH,
        )

    def relay_copy(f, side):
        return pltpu.make_async_remote_copy(
            to_row.at[f, pl.ds(in_group(2), NB)], relay.at[f, side],
            z_send_sem.at[f * 3 + 1], relay_sem.at[2 * f + side],
            device_id=peer_b, device_id_type=MESH,
        )

    def on_copy(f, side):
        return pltpu.make_async_remote_copy(
            relay.at[f, side], via.at[f, 1, pl.ds(0, NB)],
            on_sem.at[2 * f + side], z_recv_sem.at[f * 3 + 1],
            device_id=peer_a if side else peer_b, device_id_type=MESH,
        )

    odd = lax.rem(group, 2) == 1

    def start_far(f):
        @pl.when(odd)
        def _():
            far_copy(f).start()

        @pl.when(jnp.logical_not(odd))
        def _():
            z_copy(f, 2).start()

    def start_relay(f):
        @pl.when(odd)
        def _():
            relay_copy(f, group // 2).start()

    def send_on(f):
        @pl.when(group == 2)
        def _():
            for side in range(2):
                relay_copy(f, side).wait_recv()
                on_copy(f, side).start()

    def send_plane(f, step):
        source = in_group(GROUPS - step) + place if step else row

        def block(q):
            return via.at[f, step - 1, q] if step else to_row.at[f, row - place + q]

        @pl.loop(1, plane)
        def _(i):
            q = lax.rem(place + i, plane)
            pltpu.make_async_remote_copy(
                block(q), from_row.at[f, source], send_sem.at[f], recv_sem.at[f],
                device_id=(in_group(0) + q, col), device_id_type=MESH,
            ).start()

        from_row[f, source] = block(place)[...]

    def all_rows(f):
        count = GROUPS * (plane - 1)
        return pltpu.make_async_remote_copy(
            to_row.at[f, pl.ds(0, count)], from_row.at[f, pl.ds(0, count)],
            send_sem.at[f], recv_sem.at[f],
            device_id=(in_group(1) + place, col), device_id_type=MESH,
        )

    def second(f):
        lines = from_row[f].reshape(rows * 8, 256)
        modes = product((h[0], h[1]), halves(lines), ((1,), (0,)))
        for part in range(2):
            lanes = slice(128 * part, 128 * part + 128)
            to_col[f, part] = modes[:, lanes].reshape(cols, 64, 128)
            from_col[f, part, col] = to_col[f, part, col]

    def send_cols(f, part):
        for i in range(1, cols):
            peer = lax.rem(col + i, cols)
            pltpu.make_async_remote_copy(
                to_col.at[f, part, peer], from_col.at[f, part, col],
                send_sem.at[2 + 2 * f + part], recv_sem.at[2 + 2 * f + part],
                device_id=(row, peer), device_id_type=MESH,
            ).start()

    def all_cols(f, part):
        return pltpu.make_async_remote_copy(
            to_col.at[f, part, pl.ds(0, cols - 1)],
            from_col.at[f, part, pl.ds(0, cols - 1)],
            send_sem.at[2 + 2 * f + part], recv_sem.at[2 + 2 * f + part],
            device_id=(row, lax.rem(col + 1, cols)), device_id_type=MESH,
        )

    def third(f, part):
        for g in range(8):
            at = slice(8 * g, 8 * g + 8)
            for j in range(2):
                v = swap_four([from_col[f, part, 4 * j + c, at] for c in range(4)])
                for k in range(4):
                    line[k, at, 128 * j : 128 * j + 128] = v[k]

        lines = line[...].reshape(256, 256)
        modes = product(halves(lines), (hz[0], hz[1]), ((1,), (0,)))
        out[f, 4 * part : 4 * part + 4] = modes.reshape(4, 64, 256)

    @pl.when(jnp.logical_and(group != 2, n_lower + n_before > 0))
    def _():
        pl.semaphore_wait(barrier, n_lower + n_before)
        answer()

    loads[0].wait()
    for load in loads[2:]:
        load.start()
    split(0)
    loads[1].wait()
    first(0, step_a)

    @pl.when(group == 2)
    def _():
        pl.semaphore_wait(barrier, n_lower + n_before)
        answer()

    @pl.when(group == 0)
    def _():
        pl.semaphore_wait(ready_sem.at[0], 1)

    z_copy(0, step_a).start()
    loads[2].wait()
    first(0, step_b)
    loads[3].wait()
    first(0, 2)

    @pl.when(group != 2)
    def _():
        pl.semaphore_wait(ready_sem.at[1], 1)

    start_relay(0)
    z_copy(0, step_b).start()
    for peer in (peer_a, peer_b):
        signal(ready_sem.at[2], peer)

    @pl.when(n_adjacent > n_before)
    def _():
        pl.semaphore_wait(round_sem.at[3], n_adjacent - n_before)

    tell(0)
    loads[4].wait()
    first(0, 0)
    hear(0)
    tell(1)
    loads[5].wait()
    split(1)
    first(1, step_a)
    hear(1)
    tell(2)
    pl.semaphore_wait(ready_sem.at[2], 2)
    start_far(0)
    send_on(0)
    z_copy(1, step_a).start()
    first(1, step_b)
    first(1, 2)
    start_relay(1)
    z_copy(1, step_b).start()
    start_far(1)
    first(1, 0)
    hear(2)
    send_plane(0, 0)
    send_plane(1, 0)
    loads[6].wait()
    for f in range(2):
        for step in (*near, 2):
            z_copy(f, step).wait_recv()
            send_plane(f, step)
        if f == 0:
            send_on(1)
        all_rows(f).wait_recv()
        second(f)
        for part in range(2):
            send_cols(f, part)
    for f in range(2):
        for part in range(2):
            all_cols(f, part).wait_recv()
            third(f, part)
    for f in range(2):
        for step in (*near, 2):
            z_copy(f, step).wait_send()
        all_rows(f).wait_send()
        for part in range(2):
            all_cols(f, part).wait_send()

        @pl.when(group == 2)
        def _():
            for side in range(2):
                on_copy(f, side).wait_send()


def divide(spectrum, sx, sy, sz, out, done, sems):
    row, col = lax.axis_index("row"), lax.axis_index("col")
    fields, share_x, share_y, nz = spectrum.shape
    lane = lax.broadcasted_iota(jnp.int32, (share_y, sy.shape[1]), 1)
    sub = lax.broadcasted_iota(jnp.int32, (share_y, sy.shape[1]), 0)
    mine = lane == col * share_y + sub
    part_y = jnp.sum(jnp.where(mine, sy[...], 0.0), axis=1, keepdims=True)
    lane_x = lax.broadcasted_iota(jnp.int32, sx.shape, 1)
    copies = []
    for k in range(share_x):
        mine = lane_x == row * share_x + k
        part_x = jnp.sum(jnp.where(mine, sx[...], 0.0), axis=1, keepdims=True)
        symbol = (part_x + part_y) + sz[...]
        for f in range(fields):
            done[f, k] = spectrum[f, k] / symbol
        if k % 2 == 1:
            two = pl.ds(k - 1, 2)
            copies.append(
                pltpu.make_async_copy(done.at[:, two], out.at[:, two], sems.at[k // 2])
            )
            copies[-1].start()
    for copy in copies:
        copy.wait()


def on_device(rows, cols, species, symbol_x, symbol_y, symbol_z):
    fields, nx, ny, nz = species.shape
    values = species.transpose(0, 2, 3, 1).reshape(fields, ny * nz, nx)
    table_z = np.pad(split_table(nz * cols), ((0, 0), (0, 0), (0, nx - nz * cols)))
    table = jnp.asarray(np.concatenate([split_table(nx), table_z], axis=1))
    share_x, share_y = nx // rows, ny * rows // cols
    in_hbm = pl.BlockSpec(memory_space=pltpu.HBM)
    in_vmem = pl.BlockSpec(memory_space=pltpu.VMEM)
    result = jax.ShapeDtypeStruct((fields, share_x, share_y, nz * cols), F32)
    spectrum = pl.pallas_call(
        functools.partial(kernel, rows, cols),
        out_shape=result,
        in_specs=[in_hbm] * 2,
        out_specs=in_vmem,
        scratch_shapes=[
            pltpu.VMEM(values.shape, F32),
            pltpu.VMEM((fields, 2, ny * nz, nx), BF16),
            pltpu.VMEM((2, nx, nx), BF16),
            pltpu.VMEM((2, nz * cols, nz * cols), BF16),
            pltpu.VMEM((nx // GROUPS, ny * nz), F32),
            pltpu.VMEM((fields, rows, 8, 256), F32),
            pltpu.VMEM((fields, GROUPS - 1, rows // GROUPS, 8, 256), F32),
            pltpu.VMEM((fields, 2, NB, 8, 256), F32),
            pltpu.VMEM((fields, rows, 8, 256), F32),
            pltpu.VMEM((fields, 2, cols, 64, 128), F32),
            pltpu.VMEM((fields, 2, cols, 64, 128), F32),
            pltpu.VMEM((4, 64, 256), F32),
            pltpu.SemaphoreType.DMA((7,)),
            pltpu.SemaphoreType.DMA((6,)),
            pltpu.SemaphoreType.DMA((6,)),
            pltpu.SemaphoreType.DMA((6,)),
            pltpu.SemaphoreType.DMA((6,)),
            pltpu.SemaphoreType.DMA((4,)),
            pltpu.SemaphoreType.DMA((4,)),
            pltpu.SemaphoreType.REGULAR((3,)),
            pltpu.SemaphoreType.REGULAR((4,)),
        ],
        compiler_params=pltpu.CompilerParams(
            collective_id=0, has_side_effects=True, vmem_limit_bytes=VMEM_LIMIT
        ),
    )(values, table)
    return pl.pallas_call(
        divide,
        out_shape=result,
        in_specs=[in_vmem] * 4,
        out_specs=in_hbm,
        scratch_shapes=[
            pltpu.VMEM(result.shape, F32),
            pltpu.SemaphoreType.DMA((share_x // 2,)),
        ],
        compiler_params=pltpu.CompilerParams(vmem_limit_bytes=8 * 2**20),
    )(spectrum, symbol_x[None], symbol_y[None], symbol_z[None])


def solution(mesh):
    in_specs = (P(None, None, "row", "col"), P(), P(), P())
    out_specs = P(None, "row", "col", None)
    return jax.shard_map(
        functools.partial(on_device, mesh.shape["row"], mesh.shape["col"]),
        mesh=mesh, in_specs=in_specs, out_specs=out_specs, check_vma=False,
    )
```

```python
import functools

import jax
import jax.numpy as jnp
import ml_dtypes
import numpy as np
from jax import lax
from jax.experimental import pallas as pl
from jax.experimental.pallas import tpu as pltpu
from jax.sharding import PartitionSpec as P

MESH = pl.DeviceIdType.MESH
F32 = jnp.float32
BF16 = jnp.bfloat16
GROUPS = 4
NB = 4
VMEM_LIMIT = 53500 * 2**10


def split_table(count):
    rank = np.arange(count, dtype=np.float64)
    angle = np.pi / (4 * count) * (2 * rank[:, None] + 1) * (2 * rank[None, :] + 1)
    table = (np.cos(angle) * np.sqrt(2.0 / count)).astype(np.float32)
    high = table.astype(ml_dtypes.bfloat16)
    low = (table - high.astype(np.float32)).astype(ml_dtypes.bfloat16)
    return np.stack([high, low])


def halves(values):
    high = values.astype(BF16)
    return high, (values - high.astype(F32)).astype(BF16)


def product(a, b, dims):
    dot = functools.partial(
        lax.dot_general, dimension_numbers=(dims, ((), ())), preferred_element_type=F32
    )
    return dot(a[0], b[0]) + dot(a[0], b[1]) + dot(a[1], b[0])


def swap_granules(v0, v1):
    sub = lax.broadcasted_iota(jnp.int32, (8, 128), 0)
    lane = lax.broadcasted_iota(jnp.int32, (8, 128), 1)
    upper = sub >= 4
    w0 = jnp.where(upper, pltpu.roll(v1, 4, 0), v0)
    w1 = jnp.where(upper, v1, pltpu.roll(v0, 4, 0))
    s1, g1 = (sub // 2) % 2, lane // 64
    s0, g0 = sub % 2, (lane // 32) % 2
    out = []
    for w in (w0, w1):
        u = pltpu.roll(w, 64, 1)
        w = jnp.where(
            s1 == g1, w, jnp.where(s1 == 0, pltpu.roll(u, 6, 0), pltpu.roll(u, 2, 0))
        )
        a, b = pltpu.roll(w, 32, 1), pltpu.roll(w, 96, 1)
        w = jnp.where(
            s0 == g0, w, jnp.where(s0 == 0, pltpu.roll(a, 7, 0), pltpu.roll(b, 1, 0))
        )
        out.append(w)
    return out


def swap_four(v):
    lane = lax.broadcasted_iota(jnp.int32, (8, 128), 1)
    g1, g0 = lane // 64 == 1, (lane // 32) % 2 == 1
    w = [None] * 4
    for k in range(2):
        a, b = v[k], v[k + 2]
        w[k] = jnp.where(g1, pltpu.roll(b, 64, 1), a)
        w[k + 2] = jnp.where(g1, b, pltpu.roll(a, 64, 1))
    o = [None] * 4
    for k in (0, 2):
        a, b = w[k], w[k + 1]
        o[k] = jnp.where(g0, pltpu.roll(b, 32, 1), a)
        o[k + 1] = jnp.where(g0, b, pltpu.roll(a, 96, 1))
    return o


def kernel(
    rows, cols, x_hbm, h_hbm, out, x, xs, h, hz, mid, to_row, via, relay, from_row, to_col, from_col, line,
    load_sem, send_sem, recv_sem, z_send_sem, z_recv_sem, relay_sem, on_sem,
    ready_sem, round_sem,
):
    row, col = lax.axis_index("row"), lax.axis_index("col")
    plane = rows // GROUPS
    group, place = row // plane, lax.rem(row, plane)

    def in_group(step):
        return lax.rem(group + step, GROUPS) * plane

    def signal(semaphore, peer):
        pl.semaphore_signal(semaphore, inc=1, device_id=peer, device_id_type=MESH)

    def in_plane(x_step, y_step):
        x = lax.rem(lax.rem(place, 4) + x_step, 4)
        y = lax.rem(place // 4 + y_step, 4)
        return row - place + 4 * y + x, col

    flip = lax.rem(group % 2 + group // 2, 2)
    step_a, step_b = 1 + 2 * flip, 3 - 2 * flip
    peer_a = (in_group(step_a) + place, col)
    peer_b = (in_group(step_b) + place, col)
    z_lo, core = col // 2, lax.rem(col, 2)
    x_at, y_at = lax.rem(place, 4), place // 4
    adjacent = [
        (x_at < 3, in_plane(1, 0)),
        (x_at == 0, in_plane(3, 0)),
        (y_at < 3, in_plane(0, 1)),
        (y_at == 0, in_plane(0, 3)),
        (core == 0, (row, col + 1 - 2 * core)),
    ]
    n_adjacent = len(adjacent) + 1 + z_lo * (3 - z_lo) // 2
    n_before = (x_at + 1) // 2 + (y_at + 1) // 2 + core + (z_lo + 3) // 4

    def signal_adjacent(semaphore, later, earlier):
        for is_later, peer in adjacent:
            if later and earlier:
                signal(semaphore, peer)
            else:

                @pl.when(is_later if later else jnp.logical_not(is_later))
                def _():
                    signal(semaphore, peer)

        if earlier:

            @pl.when(z_lo > 0)
            def _():
                signal(semaphore, (row, col - 2))

        if later:

            @pl.when(z_lo < 3)
            def _():
                signal(semaphore, (row, col + 2))

    barrier = pltpu.get_barrier_semaphore()
    n_lower = group % 2 + 2 * (group // 2) * (1 - group % 2)

    @pl.when(group == 0)
    def _():
        signal(barrier, peer_a)

    @pl.when(group != 2)
    def _():
        signal(barrier, peer_b)

    signal_adjacent(barrier, True, False)

    def answer():
        @pl.when(group == 1)
        def _():
            signal(ready_sem.at[0], peer_a)

        @pl.when(group >= 2)
        def _():
            signal(ready_sem.at[1], peer_a)

        @pl.when(group == 2)
        def _():
            signal(ready_sem.at[1], peer_b)

        signal_adjacent(round_sem.at[3], False, True)

    def tell(k):
        signal_adjacent(round_sem.at[k], True, True)

    def hear(k):
        pl.semaphore_wait(round_sem.at[k], n_adjacent)

    def table_part(step):
        at = pl.ds(pl.multiple_of(in_group(step) * 8, 128), plane * 8)
        return h_hbm.at[:, at, :], h.at[:, at, :]

    near = (1, GROUPS - 1)
    sources = [
        (x_hbm.at[0], x.at[0]),
        table_part(step_a),
        table_part(step_b),
        table_part(2),
        table_part(0),
        (x_hbm.at[1], x.at[1]),
        (h_hbm.at[:, pl.ds(x.shape[2], hz.shape[1]), pl.ds(0, hz.shape[1])], hz),
    ]
    loads = [
        pltpu.make_async_copy(src, dst, load_sem.at[k])
        for k, (src, dst) in enumerate(sources)
    ]
    for load in loads[:2]:
        load.start()

    def first(f, step):
        top = pl.multiple_of(in_group(step) * 8, 128)
        at = pl.ds(top, plane * 8)
        mid[...] = product((h[0, at], h[1, at]), (xs[f, 0], xs[f, 1]), ((1,), (1,)))

        for q in range(plane):
            v = swap_granules(mid[8 * q : 8 * q + 8, :128], mid[8 * q : 8 * q + 8, 128:])
            to_row[f, in_group(step) + q, :, :128] = v[0]
            to_row[f, in_group(step) + q, :, 128:] = v[1]

    def split(f):
        xs[f, 0], xs[f, 1] = halves(x[f])

    def z_copy(f, step):
        k = f * 3 + step - 1
        return pltpu.make_async_remote_copy(
            to_row.at[f, pl.ds(in_group(step), plane)], via.at[f, step - 1],
            z_send_sem.at[k], z_recv_sem.at[k],
            device_id=(in_group(step) + place, col), device_id_type=MESH,
        )

    def far_copy(f):
        return pltpu.make_async_remote_copy(
            to_row.at[f, pl.ds(in_group(2) + NB, plane - NB)], via.at[f, 1, pl.ds(NB, plane - NB)],
            z_send_sem.at[f * 3 + 1], z_recv_sem.at[f * 3 + 1],
            device_id=(in_group(2) + place, col), device_id_type=MESH,
        )

    def relay_copy(f, side):
        return pltpu.make_async_remote_copy(
            to_row.at[f, pl.ds(in_group(2), NB)], relay.at[f, side],
            z_send_sem.at[f * 3 + 1], relay_sem.at[2 * f + side],
            device_id=peer_b, device_id_type=MESH,
        )

    def on_copy(f, side):
        return pltpu.make_async_remote_copy(
            relay.at[f, side], via.at[f, 1, pl.ds(0, NB)],
            on_sem.at[2 * f + side], z_recv_sem.at[f * 3 + 1],
            device_id=peer_a if side else peer_b, device_id_type=MESH,
        )

    odd = lax.rem(group, 2) == 1

    def start_far(f):
        @pl.when(odd)
        def _():
            far_copy(f).start()

        @pl.when(jnp.logical_not(odd))
        def _():
            z_copy(f, 2).start()

    def start_relay(f):
        @pl.when(odd)
        def _():
            relay_copy(f, group // 2).start()

    def send_on(f):
        @pl.when(group == 2)
        def _():
            for side in range(2):
                relay_copy(f, side).wait_recv()
                on_copy(f, side).start()

    def send_plane(f, step):
        source = in_group(GROUPS - step) + place if step else row

        def block(q):
            return via.at[f, step - 1, q] if step else to_row.at[f, row - place + q]

        @pl.loop(1, plane)
        def _(i):
            q = lax.rem(place + i, plane)
            pltpu.make_async_remote_copy(
                block(q), from_row.at[f, source], send_sem.at[f], recv_sem.at[f],
                device_id=(in_group(0) + q, col), device_id_type=MESH,
            ).start()

        from_row[f, source] = block(place)[...]

    def all_rows(f):
        count = GROUPS * (plane - 1)
        return pltpu.make_async_remote_copy(
            to_row.at[f, pl.ds(0, count)], from_row.at[f, pl.ds(0, count)],
            send_sem.at[f], recv_sem.at[f],
            device_id=(in_group(1) + place, col), device_id_type=MESH,
        )

    def second(f):
        lines = from_row[f].reshape(rows * 8, 256)
        modes = product((h[0], h[1]), halves(lines), ((1,), (0,)))
        for part in range(2):
            lanes = slice(128 * part, 128 * part + 128)
            to_col[f, part] = modes[:, lanes].reshape(cols, 64, 128)
            from_col[f, part, col] = to_col[f, part, col]

    def send_cols(f, part):
        for i in range(1, cols):
            peer = lax.rem(col + i, cols)
            pltpu.make_async_remote_copy(
                to_col.at[f, part, peer], from_col.at[f, part, col],
                send_sem.at[2 + 2 * f + part], recv_sem.at[2 + 2 * f + part],
                device_id=(row, peer), device_id_type=MESH,
            ).start()

    def all_cols(f, part):
        return pltpu.make_async_remote_copy(
            to_col.at[f, part, pl.ds(0, cols - 1)],
            from_col.at[f, part, pl.ds(0, cols - 1)],
            send_sem.at[2 + 2 * f + part], recv_sem.at[2 + 2 * f + part],
            device_id=(row, lax.rem(col + 1, cols)), device_id_type=MESH,
        )

    def third(f, part):
        for g in range(8):
            at = slice(8 * g, 8 * g + 8)
            for j in range(2):
                v = swap_four([from_col[f, part, 4 * j + c, at] for c in range(4)])
                for k in range(4):
                    line[k, at, 128 * j : 128 * j + 128] = v[k]

        lines = line[...].reshape(256, 256)
        modes = product(halves(lines), (hz[0], hz[1]), ((1,), (0,)))
        out[f, 4 * part : 4 * part + 4] = modes.reshape(4, 64, 256)

    @pl.when(jnp.logical_and(group != 2, n_lower + n_before > 0))
    def _():
        pl.semaphore_wait(barrier, n_lower + n_before)
        answer()

    loads[0].wait()
    for load in loads[2:]:
        load.start()
    split(0)
    loads[1].wait()
    first(0, step_a)

    @pl.when(group == 2)
    def _():
        pl.semaphore_wait(barrier, n_lower + n_before)
        answer()

    @pl.when(group == 0)
    def _():
        pl.semaphore_wait(ready_sem.at[0], 1)

    z_copy(0, step_a).start()
    loads[2].wait()
    first(0, step_b)
    loads[3].wait()
    first(0, 2)

    @pl.when(group != 2)
    def _():
        pl.semaphore_wait(ready_sem.at[1], 1)

    start_relay(0)
    z_copy(0, step_b).start()
    for peer in (peer_a, peer_b):
        signal(ready_sem.at[2], peer)

    @pl.when(n_adjacent > n_before)
    def _():
        pl.semaphore_wait(round_sem.at[3], n_adjacent - n_before)

    tell(0)
    loads[4].wait()
    first(0, 0)
    hear(0)
    tell(1)
    loads[5].wait()
    split(1)
    first(1, step_a)
    hear(1)
    tell(2)
    pl.semaphore_wait(ready_sem.at[2], 2)
    start_far(0)
    send_on(0)
    z_copy(1, step_a).start()
    first(1, step_b)
    first(1, 2)
    start_relay(1)
    z_copy(1, step_b).start()
    start_far(1)
    first(1, 0)
    hear(2)
    send_plane(0, 0)
    send_plane(1, 0)
    loads[6].wait()
    for f in range(2):
        for step in (*near, 2):
            z_copy(f, step).wait_recv()
            send_plane(f, step)
        if f == 0:
            send_on(1)
        all_rows(f).wait_recv()
        second(f)
        for part in range(2):
            send_cols(f, part)
    for f in range(2):
        for part in range(2):
            all_cols(f, part).wait_recv()
            third(f, part)
    for f in range(2):
        for step in (*near, 2):
            z_copy(f, step).wait_send()
        all_rows(f).wait_send()
        for part in range(2):
            all_cols(f, part).wait_send()

        @pl.when(group == 2)
        def _():
            for side in range(2):
                on_copy(f, side).wait_send()


def divide(spectrum, sx, sy, sz, out, done, sems):
    row, col = lax.axis_index("row"), lax.axis_index("col")
    fields, share_x, share_y, nz = spectrum.shape
    lane = lax.broadcasted_iota(jnp.int32, (share_y, sy.shape[1]), 1)
    sub = lax.broadcasted_iota(jnp.int32, (share_y, sy.shape[1]), 0)
    mine = lane == col * share_y + sub
    part_y = jnp.sum(jnp.where(mine, sy[...], 0.0), axis=1, keepdims=True)
    lane_x = lax.broadcasted_iota(jnp.int32, sx.shape, 1)
    copies = []
    for k in range(share_x):
        mine = lane_x == row * share_x + k
        part_x = jnp.sum(jnp.where(mine, sx[...], 0.0), axis=1, keepdims=True)
        symbol = (part_x + part_y) + sz[...]
        for f in range(fields):
            done[f, k] = spectrum[f, k] / symbol
        copies.append(pltpu.make_async_copy(done.at[:, k], out.at[:, k], sems.at[k]))
        copies[-1].start()
    for copy in copies:
        copy.wait()


def on_device(rows, cols, species, symbol_x, symbol_y, symbol_z):
    fields, nx, ny, nz = species.shape
    values = species.transpose(0, 2, 3, 1).reshape(fields, ny * nz, nx)
    table_z = np.pad(split_table(nz * cols), ((0, 0), (0, 0), (0, nx - nz * cols)))
    table = jnp.asarray(np.concatenate([split_table(nx), table_z], axis=1))
    share_x, share_y = nx // rows, ny * rows // cols
    in_hbm = pl.BlockSpec(memory_space=pltpu.HBM)
    in_vmem = pl.BlockSpec(memory_space=pltpu.VMEM)
    result = jax.ShapeDtypeStruct((fields, share_x, share_y, nz * cols), F32)
    spectrum = pl.pallas_call(
        functools.partial(kernel, rows, cols),
        out_shape=result,
        in_specs=[in_hbm] * 2,
        out_specs=in_vmem,
        scratch_shapes=[
            pltpu.VMEM(values.shape, F32),
            pltpu.VMEM((fields, 2, ny * nz, nx), BF16),
            pltpu.VMEM((2, nx, nx), BF16),
            pltpu.VMEM((2, nz * cols, nz * cols), BF16),
            pltpu.VMEM((nx // GROUPS, ny * nz), F32),
            pltpu.VMEM((fields, rows, 8, 256), F32),
            pltpu.VMEM((fields, GROUPS - 1, rows // GROUPS, 8, 256), F32),
            pltpu.VMEM((fields, 2, NB, 8, 256), F32),
            pltpu.VMEM((fields, rows, 8, 256), F32),
            pltpu.VMEM((fields, 2, cols, 64, 128), F32),
            pltpu.VMEM((fields, 2, cols, 64, 128), F32),
            pltpu.VMEM((4, 64, 256), F32),
            pltpu.SemaphoreType.DMA((7,)),
            pltpu.SemaphoreType.DMA((6,)),
            pltpu.SemaphoreType.DMA((6,)),
            pltpu.SemaphoreType.DMA((6,)),
            pltpu.SemaphoreType.DMA((6,)),
            pltpu.SemaphoreType.DMA((4,)),
            pltpu.SemaphoreType.DMA((4,)),
            pltpu.SemaphoreType.REGULAR((3,)),
            pltpu.SemaphoreType.REGULAR((4,)),
        ],
        compiler_params=pltpu.CompilerParams(
            collective_id=0, has_side_effects=True, vmem_limit_bytes=VMEM_LIMIT
        ),
    )(values, table)
    return pl.pallas_call(
        divide,
        out_shape=result,
        in_specs=[in_vmem] * 4,
        out_specs=in_hbm,
        scratch_shapes=[
            pltpu.VMEM(result.shape, F32),
            pltpu.SemaphoreType.DMA((share_x,)),
        ],
        compiler_params=pltpu.CompilerParams(vmem_limit_bytes=8 * 2**20),
    )(spectrum, symbol_x[None], symbol_y[None], symbol_z[None])


def solution(mesh):
    in_specs = (P(None, None, "row", "col"), P(), P(), P())
    out_specs = P(None, "row", "col", None)
    return jax.shard_map(
        functools.partial(on_device, mesh.shape["row"], mesh.shape["col"]),
        mesh=mesh, in_specs=in_specs, out_specs=out_specs, check_vma=False,
    )
```
